32 devices in a mesh: tp: 4 (over z), dp: 8 (over y, x, core).
Axes of the slice: x: 2, y: 2, z: 4, core: 2. Of those that a mesh axis runs over, the one named last changes fastest.
Arguments:
- w_query: bfloat16 [1024, 1024], P(('dp', 'tp'))
- b_query: bfloat16 [1024], P(('dp', 'tp'))
- w_key: bfloat16 [1024, 1024], P(('dp', 'tp'))
- b_key: bfloat16 [1024], P(('dp', 'tp'))
- w_value: bfloat16 [1024, 1024], P(('dp', 'tp'))
- b_value: bfloat16 [1024], P(('dp', 'tp'))
- w_out: bfloat16 [1024, 1024], P(('dp', 'tp'))
- w_gate: bfloat16 [2816, 1024], P(('dp', 'tp'))
- w_up: bfloat16 [2816, 1024], P(('dp', 'tp'))
- w_down: bfloat16 [1024, 2816], P(('dp', 'tp'))
- gain_attn: bfloat16 [1024], P(('dp', 'tp'))
- gain_mlp: bfloat16 [1024], P(('dp', 'tp'))
- hidden: bfloat16 [2048, 1024], P('dp')
- k_cache: bfloat16 [2048, 64, 16, 64], P('dp', None, 'tp')
- v_cache: bfloat16 [2048, 64, 16, 64], P('dp', None, 'tp')
- lengths: int32 [2048], P('dp')
Outputs:
- output 1: bfloat16 [1024, 1024], P('tp')
- output 2: bfloat16 [1024], P('tp')
- output 3: bfloat16 [1024, 1024], P('tp')
- output 4: bfloat16 [1024], P('tp')
- output 5: bfloat16 [1024, 1024], P('tp')
- output 6: bfloat16 [1024], P('tp')
- output 7: bfloat16 [1024, 1024], P(None, 'tp')
- output 8: bfloat16 [2816, 1024], P('tp')
- output 9: bfloat16 [2816, 1024], P('tp')
- output 10: bfloat16 [1024, 2816], P(None, 'tp')
- output 11: bfloat16 [1024], replicated
- output 12: bfloat16 [1024], replicated
- output 13: bfloat16 [2048, 1024], P('dp')
- output 14: bfloat16 [2048, 64, 16, 64], P('dp', None, 'tp')
- output 15: bfloat16 [2048, 64, 16, 64], P('dp', None, 'tp')
All inputs are finite; a program needn't handle non-finite values.
Results may differ from the reference program's by a relative error of at most 0.013719.
Values are sent between devices in bfloat16 or wider.
A program may use at most 1 GiB of HBM per device.

```python
import jax
import jax.numpy as jnp
from jax import lax

HIDDEN = 1024
Q_HEADS = 16
KV_HEADS = 16
HEAD_DIM = 64
FF_DIM = 2816
TP_SIZE = 4
DP_SIZE = 8
ROLLOUTS = 256
CACHE_LEN = 64

BATCH = DP_SIZE * ROLLOUTS
KV_SLOTS = max(KV_HEADS, TP_SIZE)
REPEATS = KV_SLOTS // KV_HEADS
Q_ROWS = Q_HEADS * HEAD_DIM
KV_ROWS = KV_HEADS * HEAD_DIM
EPS = 1e-6
THETA = 1000000.0


def draw_lengths(key_a, key_b):
    first_draw = jax.random.randint(key_a, (BATCH,), 0, CACHE_LEN)
    second_draw = jax.random.randint(key_b, (BATCH,), 0, CACHE_LEN)
    lengths = 1 + (first_draw * second_draw) // CACHE_LEN
    row_index = jnp.arange(BATCH)
    lengths = jnp.where(row_index == 0, CACHE_LEN - 1, lengths)
    return jnp.where(row_index == 1, 1, lengths).astype(jnp.int32)


def setup_inputs(seed: int = 0) -> dict:
    keys = jax.random.split(jax.random.key(seed), 17)

    def normal_bf16(key_index, shape, scale):
        return (jax.random.normal(keys[key_index], shape, jnp.float32) * scale).astype(jnp.bfloat16)

    def gain_bf16(key_index):
        return (1.0 + 0.3 * jax.random.normal(keys[key_index], (HIDDEN,), jnp.float32)).astype(jnp.bfloat16)

    k_base = jax.random.normal(keys[13], (BATCH, CACHE_LEN, KV_HEADS, HEAD_DIM), jnp.float32)
    v_base = jax.random.normal(keys[14], (BATCH, CACHE_LEN, KV_HEADS, HEAD_DIM), jnp.float32)
    return {
        "w_query": normal_bf16(0, (Q_ROWS, HIDDEN), 3.0 * HIDDEN ** -0.5),
        "b_query": normal_bf16(1, (Q_ROWS,), 1.0),
        "w_key": normal_bf16(2, (KV_ROWS, HIDDEN), HIDDEN ** -0.5),
        "b_key": normal_bf16(3, (KV_ROWS,), 0.5),
        "w_value": normal_bf16(4, (KV_ROWS, HIDDEN), HIDDEN ** -0.5),
        "b_value": normal_bf16(5, (KV_ROWS,), 0.5),
        "w_out": normal_bf16(6, (HIDDEN, Q_ROWS), Q_ROWS ** -0.5),
        "w_gate": normal_bf16(7, (FF_DIM, HIDDEN), HIDDEN ** -0.5),
        "w_up": normal_bf16(8, (FF_DIM, HIDDEN), HIDDEN ** -0.5),
        "w_down": normal_bf16(9, (HIDDEN, FF_DIM), FF_DIM ** -0.5),
        "gain_attn": gain_bf16(10),
        "gain_mlp": gain_bf16(11),
        "hidden": normal_bf16(12, (BATCH, HIDDEN), 1.0),
        "k_cache": jnp.repeat(k_base, REPEATS, axis=2).astype(jnp.bfloat16),
        "v_cache": jnp.repeat(v_base, REPEATS, axis=2).astype(jnp.bfloat16),
        "lengths": draw_lengths(keys[15], keys[16]),
    }


def rms_scale(act_rows, gain_vec):
    rows_f32 = act_rows.astype(jnp.float32)
    inv_rms = lax.rsqrt(jnp.mean(rows_f32 * rows_f32, axis=-1, keepdims=True) + EPS)
    return (rows_f32 * inv_rms * gain_vec.astype(jnp.float32)).astype(jnp.bfloat16)


def linear_bias(act_rows, weight, bias_vec):
    result = jnp.dot(act_rows, weight.T, preferred_element_type=jnp.float32)
    return (result + bias_vec.astype(jnp.float32)).astype(jnp.bfloat16)


def linear_plain(act_rows, weight):
    return jnp.dot(act_rows, weight.T, preferred_element_type=jnp.float32).astype(jnp.bfloat16)


def rotary(vectors, positions):
    half_dim = HEAD_DIM // 2
    inv_freq = 1.0 / (THETA ** (jnp.arange(0, HEAD_DIM, 2, dtype=jnp.float32) / HEAD_DIM))
    angles = positions.astype(jnp.float32)[:, None] * inv_freq[None, :]
    cosine = jnp.cos(angles)[:, None, :]
    sine_tab = jnp.sin(angles)[:, None, :]
    vectors_f32 = vectors.astype(jnp.float32)
    first_half = vectors_f32[..., :half_dim]
    second_half = vectors_f32[..., half_dim:]
    return jnp.concatenate([first_half * cosine - second_half * sine_tab, second_half * cosine + first_half * sine_tab], axis=-1).astype(jnp.bfloat16)


def attend_block(block):
    query_block, keys_block, values_block, lens_block = block
    grouped = query_block.reshape(ROLLOUTS, KV_SLOTS, Q_HEADS // KV_SLOTS, HEAD_DIM).astype(jnp.float32)
    scores = jnp.einsum("bkgd,bskd->bkgs", grouped, keys_block.astype(jnp.float32)) * HEAD_DIM ** -0.5
    visible = (jnp.arange(CACHE_LEN)[None, :] <= lens_block[:, None])[:, None, None, :]
    attn_probs = jax.nn.softmax(jnp.where(visible, scores, -1e30), axis=-1).astype(jnp.bfloat16)
    mixed = jnp.einsum("bkgs,bskd->bkgd", attn_probs.astype(jnp.float32), values_block.astype(jnp.float32))
    return mixed.astype(jnp.bfloat16).reshape(ROLLOUTS, Q_ROWS)


def reference(w_query, b_query, w_key, b_key, w_value, b_value, w_out, w_gate, w_up, w_down, gain_attn, gain_mlp, hidden, k_cache, v_cache, lengths):
    w_key_tp = jnp.repeat(w_key.reshape(KV_HEADS, HEAD_DIM, HIDDEN), REPEATS, axis=0).reshape(KV_SLOTS * HEAD_DIM, HIDDEN)
    b_key_tp = jnp.repeat(b_key.reshape(KV_HEADS, HEAD_DIM), REPEATS, axis=0).reshape(KV_SLOTS * HEAD_DIM)
    w_value_tp = jnp.repeat(w_value.reshape(KV_HEADS, HEAD_DIM, HIDDEN), REPEATS, axis=0).reshape(KV_SLOTS * HEAD_DIM, HIDDEN)
    b_value_tp = jnp.repeat(b_value.reshape(KV_HEADS, HEAD_DIM), REPEATS, axis=0).reshape(KV_SLOTS * HEAD_DIM)
    normed = rms_scale(hidden, gain_attn)
    query_rot = rotary(linear_bias(normed, w_query, b_query).reshape(BATCH, Q_HEADS, HEAD_DIM), lengths)
    key_rot = rotary(linear_bias(normed, w_key_tp, b_key_tp).reshape(BATCH, KV_SLOTS, HEAD_DIM), lengths)
    value_new = linear_bias(normed, w_value_tp, b_value_tp).reshape(BATCH, KV_SLOTS, HEAD_DIM)
    at_slot = (jnp.arange(CACHE_LEN)[None, :] == lengths[:, None])[:, :, None, None]
    k_cache_out = jnp.where(at_slot, key_rot[:, None], k_cache)
    v_cache_out = jnp.where(at_slot, value_new[:, None], v_cache)
    attended = lax.map(attend_block, (
        query_rot.reshape(DP_SIZE, ROLLOUTS, Q_HEADS, HEAD_DIM),
        k_cache_out.reshape(DP_SIZE, ROLLOUTS, CACHE_LEN, KV_SLOTS, HEAD_DIM),
        v_cache_out.reshape(DP_SIZE, ROLLOUTS, CACHE_LEN, KV_SLOTS, HEAD_DIM),
        lengths.reshape(DP_SIZE, ROLLOUTS))).reshape(BATCH, Q_ROWS)
    attn_proj = linear_plain(attended, w_out)
    mid_hidden = (hidden.astype(jnp.float32) + attn_proj.astype(jnp.float32)).astype(jnp.bfloat16)
    normed_mlp = rms_scale(mid_hidden, gain_mlp)
    gate_val = linear_plain(normed_mlp, w_gate)
    up_val = linear_plain(normed_mlp, w_up)
    gated = (jax.nn.silu(gate_val.astype(jnp.float32)) * up_val.astype(jnp.float32)).astype(jnp.bfloat16)
    down_val = linear_plain(gated, w_down)
    hidden_out = (mid_hidden.astype(jnp.float32) + down_val.astype(jnp.float32)).astype(jnp.bfloat16)
    return (w_query, b_query, w_key_tp, b_key_tp, w_value_tp, b_value_tp, w_out, w_gate, w_up, w_down, gain_attn, gain_mlp, hidden_out, k_cache_out, v_cache_out)
```

```python
import functools
import math

import jax
import jax.numpy as jnp
from jax import lax
from jax.experimental import pallas as pl
from jax.experimental.pallas import tpu as pltpu
from jax.sharding import PartitionSpec as P

EPS = 1e-6
THETA = 1000000.0
MESH = pl.DeviceIdType.MESH
BF16, F32 = jnp.bfloat16, jnp.float32
TP, DP = 4, 8
PEERS = TP * DP - 1
HEAD, HALF = 64, 32
WIDTH, QUARTER, LANES = 1024, 256, 128
BLOCK, WIDE_BLOCK = 32, 88
FF, FF_PAD = 704, 768
MIB = 2**20


def _place():
    z, dp = lax.axis_index("tp"), lax.axis_index("dp")
    core, col = dp % 2, dp // 2
    x, y = col % 2, col // 2
    cols = (col, col + 1 - 2 * x, col + 2 - 4 * y, 3 - col)
    peers = {"x": dp + 2 - 4 * x, "y": dp + 4 - 8 * y, "d": dp + 1 - 2 * core}
    return z, dp, core, col, cols, peers


def _remote(src, dst, send, recv, tp, dp):
    return pltpu.make_async_remote_copy(
        src_ref=src, dst_ref=dst, send_sem=send, recv_sem=recv, device_id={"tp": tp, "dp": dp}, device_id_type=MESH
    )


def _rows(start, size):
    return pl.ds(pl.multiple_of(start, 8), size)


def _lanes(start, size):
    return pl.ds(pl.multiple_of(start, 128), size)


def _signal(sem, tp, dp):
    pl.semaphore_signal(sem, inc=1, device_id={"tp": tp, "dp": dp}, device_id_type=MESH)


def _dot(a, b, ca, cb):
    return lax.dot_general(a, b, (((ca,), (cb,)), ((), ())), preferred_element_type=F32)


def _iota(shape, axis):
    return lax.broadcasted_iota(jnp.int32, shape, axis)


def _sublane(shape):
    return _iota(shape, 0)


def _lane(shape):
    return _iota(shape, 1)


def _in_hbm(array):
    return pltpu.with_memory_space_constraint(array, pltpu.HBM)


def _rms(act, gain_row):
    act = act.astype(F32)
    inv = lax.rsqrt(jnp.mean(act * act, axis=-1, keepdims=True) + EPS)
    return (act * inv * gain_row).astype(BF16)


class _Spread:
    def __init__(self, tp, dp, cols, peers, src_own, region, halves, total, send, recv):
        self.tp, self.cols, self.peers = tp, cols, peers
        self.src_own, self.region, self.halves, self.total = src_own, region, halves, total
        self.send, self.recv = send, recv
        self.sent = []

    def _go(self, src, dst, peer, recv_index):
        copy = _remote(src, dst, self.send.at[len(self.sent)], self.recv.at[recv_index], self.tp, self.peers[peer])
        copy.start()
        self.sent.append(copy)

    def _got(self, ref, recv_index):
        _remote(ref, ref, self.send.at[0], self.recv.at[recv_index], self.tp, self.peers["x"]).wait_recv()

    def first(self):
        own = self.region(self.cols[0])
        self._go(self.src_own, own, "x", 0)
        self._go(self.src_own, own, "y", 1)
        self._go(self.src_own, own, "d", 4)

    def second(self):
        at_x, at_y = self.region(self.cols[1]), self.region(self.cols[2])
        self._got(at_x, 0)
        upper = self.halves(self.cols[1], 0)
        self._go(upper, upper, "y", 2)
        self._go(at_x, at_x, "d", 4)
        self._got(at_y, 1)
        lower = self.halves(self.cols[2], 1)
        self._go(lower, lower, "x", 3)
        self._go(at_y, at_y, "d", 4)

    def third(self):
        upper, lower = self.halves(self.cols[3], 0), self.halves(self.cols[3], 1)
        self._got(upper, 2)
        self._go(upper, upper, "d", 4)
        self._got(lower, 3)
        self._go(lower, lower, "d", 4)

    def last(self):
        self._got(self.total, 4)

    def drain(self):
        for copy in self.sent:
            copy.wait_send()


SPREAD_SENDS, SPREAD_RECVS = 9, 5
Q, K, V, OUT, DOWN, GATE, UP = range(7)
ROW_SHARED = (Q, K, V, GATE, UP)


def _gather_kernel(
    wq, wk, wv, wo, wd, wg, wu, bq, bk, bv, ga, gm, hid, lens, kc, vc,
    oq, ok, ov, oo, rd, rg, ru, qt, kt, vt, obq, obk, obv, oga, ogm, hid_v, kc_v, vc_v,
    sq, sk, sv, so, sd, sg, su, tq, tk, tv, tg, tu, dcut, vecs, lens_v, aux, board, act,
    load_sem, vec_sem, own_sem, s0_send, s0_recv, s1_send, s1_recv, sp_send, sp_recv, aux_send, aux_recv,
):
    z, dp, core, col, cols, peers = _place()
    device = dp * TP + z
    own_here = z == col
    away = jnp.logical_not(own_here)
    at_peer = (dp, peers["x"], peers["y"], 2 * cols[3] + core)
    hbm = (wq, wk, wv, wo, wd, wg, wu)
    source = (sq, sk, sv, so, sd, sg, su)
    staged = {Q: tq, K: tk, V: tv, GATE: tg, UP: tu}

    loads = [pltpu.make_async_copy(src, dst, load_sem.at[i]) for i, (src, dst) in enumerate(
        zip(hbm + (hid, lens, kc, vc), source + (hid_v, lens_v, kc_v, vc_v)))]
    small = [pltpu.make_async_copy(src, vecs.at[i], vec_sem.at[i]) for i, src in enumerate((bq, bk, bv, ga, gm))]
    for copy in loads[:GATE + 2] + small + loads[GATE + 2:]:
        copy.start()

    barrier = pltpu.get_barrier_semaphore()

    @pl.loop(1, TP * DP)
    def _(k):
        other = (device + k) % (TP * DP)
        _signal(barrier, other % TP, other // TP)

    for copy in small:
        copy.wait()
    spots = [(_lane((BLOCK, LANES)) == _sublane((BLOCK, LANES)) + BLOCK * r).astype(BF16) for r in range(TP)]
    aux[0] = sum(_dot(vecs[r], spot, 1, 0) for r, spot in enumerate(spots))
    aux[1] = _dot(vecs[TP], spots[0], 1, 0)
    board[pl.ds(device, 1)] = aux[...].reshape(1, 2, 1, LANES)
    loads[DOWN].wait()
    for t in range(TP):
        dcut[t, :, :FF] = sd[:, FF * t:FF * (t + 1)]
        dcut[t, :, FF:] = jnp.zeros((BLOCK, FF_PAD - FF), BF16)
    for w in (Q, K, V, OUT, GATE, UP):
        loads[w].wait()

    pl.semaphore_wait(barrier, PEERS)

    sent = []
    guarded = []

    def lanes_of(column):
        return _lanes(column * QUARTER, QUARTER)

    def root(w, plane_row):
        rows = source[w].shape[0]
        if w in (GATE, UP):
            return lambda column: (rg if w == GATE else ru).at[_rows(plane_row * rows, rows), :]
        ref = (oq, ok, ov)[w]
        return lambda column: ref.at[_rows((core * TP + plane_row) * rows, rows), lanes_of(column)]

    def scatter(w):
        for m in (1, 2, 3):
            src = source[w].at[:, lanes_of(cols[m])]
            sems = s0_send.at[w, m], s0_recv.at[w, m], z, at_peer[m]
            landing = _remote(src, root(w, z)(cols[m]), *sems)
            passing = _remote(src, staged[w].at[m], *sems)

            @pl.when(own_here)
            def _():
                landing.start()

            @pl.when(away)
            def _():
                passing.start()
            sent.append(passing)

        @pl.when(own_here)
        def _():
            pltpu.make_async_copy(hbm[w].at[:, lanes_of(col)], root(w, z)(col), own_sem.at[w]).start()

    def forward(w):
        for m in range(4):
            piece = source[w].at[:, lanes_of(col)] if m == 0 else staged[w].at[m]
            copy = _remote(piece, root(w, z)(col), s1_send.at[w, m], s1_recv.at[w], cols[m], dp)
            if m:
                _remote(staged[w].at[m], staged[w].at[m], s0_send.at[w, m], s0_recv.at[w, m], z, dp).wait_recv()
            elsewhere = cols[m] != z

            @pl.when(elsewhere)
            def _():
                copy.start()
            guarded.append((elsewhere, copy))

    def got_root(w):
        ref = (oq, ok, ov, None, None, rg, ru)[w]
        rows = source[w].shape[0]
        _remote(ref.at[pl.ds(0, 3 * rows), pl.ds(0, QUARTER)], ref.at[pl.ds(0, 3 * rows), pl.ds(0, QUARTER)],
                s1_send.at[w, 0], s1_recv.at[w], z, peers["x"]).wait_recv()

        @pl.when(own_here)
        def _():
            pltpu.make_async_copy(hbm[w].at[:, lanes_of(col)], root(w, z)(col), own_sem.at[w]).wait()

    def columns(w, piece, dst):
        for m in (1, 2, 3):
            plane = (z + m) % TP
            copy = _remote(piece(plane), dst, s1_send.at[w, m], s1_recv.at[w], plane, dp)
            copy.start()
            sent.append(copy)

    def got_columns(w, ref):
        _remote(ref.at[pl.ds(0, 3 * BLOCK)], ref.at[pl.ds(0, 3 * BLOCK)], s1_send.at[w, 0], s1_recv.at[w], z,
                peers["x"]).wait_recv()

    for w in (Q, K, V):
        scatter(w)
    out_rows = oo.at[_rows(dp * LANES + z * BLOCK, BLOCK), :]
    out_own = pltpu.make_async_copy(wo.at[:, lanes_of(z)], out_rows, own_sem.at[OUT])
    out_own.start()
    columns(OUT, lambda plane: so.at[:, lanes_of(plane)], out_rows)

    def announce(k):
        other = (device + k) % (TP * DP)
        return _remote(aux, board.at[device], aux_send, aux_recv, other % TP, other // TP)

    @pl.loop(1, TP * DP)
    def _(k):
        announce(k).start()

    for w in (GATE, UP):
        scatter(w)

    def qkv_spread(w, ref):
        return _Spread(
            z, dp, cols, peers,
            ref.at[_rows(core * LANES, LANES), lanes_of(col)],
            lambda column: ref.at[_rows(core * LANES, LANES), lanes_of(column)],
            lambda column, half: ref.at[_rows(core * LANES + HEAD * half, HEAD), lanes_of(column)],
            ref.at[_rows((1 - core) * LANES, LANES), :],
            sp_send.at[w], sp_recv.at[w])

    spreads = [qkv_spread(Q, oq), qkv_spread(K, ok), qkv_spread(V, ov)]
    spreads.append(_Spread(
        z, dp, cols, peers,
        oo.at[_rows(dp * LANES, LANES), :],
        lambda column: oo.at[_rows((2 * column + core) * LANES, LANES), :],
        lambda column, half: oo.at[_rows((2 * column + core) * LANES + HEAD * half, HEAD), :],
        oo.at[pl.ds(0, WIDTH // 2), :],
        sp_send.at[OUT], sp_recv.at[OUT]))

    for w in (Q, K, V):
        forward(w)
    down_rows = rd.at[_rows(z * BLOCK, BLOCK), :]
    columns(DOWN, lambda plane: dcut.at[plane], down_rows)
    down_rows[...] = dcut[z]
    for w in (GATE, UP):
        forward(w)

    for w in (Q, K, V):
        got_root(w)
        spreads[w].first()
    spreads[Q].second()
    spreads[K].second()
    got_columns(OUT, oo)
    out_own.wait()
    spreads[OUT].first()
    spreads[Q].third()
    spreads[V].second()
    spreads[K].third()

    landed = board.at[pl.ds(0, PEERS)]
    _remote(landed, landed, aux_send, aux_recv, z, peers["x"]).wait_recv()
    sub = _sublane((BLOCK, LANES))
    first, second = jnp.zeros((BLOCK, LANES), F32), jnp.zeros((BLOCK, LANES), F32)
    for i in range(TP * DP):
        first = jnp.where(sub == i, board[i, 0], first)
        second = jnp.where(sub == i, board[i, 1], second)
    first, second = first.astype(BF16), second.astype(BF16)

    def spread_row(table, offset, count, keep):
        width = count * BLOCK
        spot = (_sublane((LANES, width)) == _lane((LANES, width)) % BLOCK + offset).astype(BF16)
        wide = _dot(table, spot, 1, 0)
        mine = _sublane((BLOCK, width)) == keep + _lane((BLOCK, width)) // BLOCK
        return jnp.sum(jnp.where(mine, wide, 0.0), axis=0, keepdims=True)

    gain_row = spread_row(first, 3 * BLOCK, TP * DP, 0)
    oga[...] = gain_row.astype(BF16)
    ogm[...] = spread_row(second, 0, TP * DP, 0).astype(BF16)
    for r, ref in enumerate((obq, obk, obv)):
        ref[...] = spread_row(first, BLOCK * r, DP, DP * z).astype(BF16)

    def bias_column(r):
        tall_shape = (QUARTER, BLOCK)
        pick = (_lane(tall_shape) == DP * z + _sublane(tall_shape) // BLOCK).astype(BF16)
        tall = _dot(pick, first, 1, 0)
        mine = _lane(tall.shape) == BLOCK * r + _sublane(tall.shape) % BLOCK
        return jnp.sum(jnp.where(mine, tall, 0.0), axis=1, keepdims=True)

    for copy in loads[UP + 1:UP + 3]:
        copy.wait()
    act[...] = _rms(hid_v[...], gain_row)

    inv_freq = jnp.exp(_sublane((HALF, QUARTER)).astype(F32) * (-math.log(THETA) / HALF))
    angle = lens_v[...].astype(F32) * inv_freq
    cosine, sine = jnp.cos(angle), jnp.sin(angle)

    def project(weight, r):
        return (_dot(weight[...], act[...], 1, 1) + bias_column(r)).astype(BF16)

    def rotate(vec, out):
        vec = vec.astype(F32)
        for h in range(TP):
            base = HEAD * h
            lo, hi = vec[base:base + HALF], vec[base + HALF:base + HEAD]
            out[base:base + HALF] = (lo * cosine - hi * sine).astype(BF16)
            out[base + HALF:base + HEAD] = (hi * cosine + lo * sine).astype(BF16)

    spreads[V].third()
    spreads[Q].last()
    rotate(project(oq, Q), qt)
    spreads[K].last()
    rotate(project(ok, K), kt)
    spreads[V].last()
    vt[...] = project(ov, V)

    spreads[OUT].second()
    spreads[OUT].third()
    spreads[OUT].last()
    got_columns(DOWN, rd)
    got_root(GATE)
    got_root(UP)

    for copy in loads[UP + 3:]:
        copy.wait()
    for copy in sent:
        copy.wait_send()
    for elsewhere, copy in guarded:
        @pl.when(elsewhere)
        def _():
            copy.wait_send()
    for spread in spreads:
        spread.drain()
    _remote(landed, landed, aux_send, aux_recv, z, peers["x"]).wait_send()


def _gather(weights, vectors, hid, lens, kc, vc):
    vmem = pl.BlockSpec(memory_space=pltpu.VMEM)
    anywhere = pl.BlockSpec(memory_space=pltpu.HBM)
    sizes = [(QUARTER, WIDTH)] * 3 + [(WIDTH, QUARTER), (LANES, FF_PAD)] + [(TP * WIDE_BLOCK, QUARTER)] * 2
    sizes += [(QUARTER, QUARTER)] * 3 + [(1, QUARTER)] * 3 + [(1, WIDTH)] * 2 + [hid.shape, kc.shape, vc.shape]
    dma = pltpu.SemaphoreType.DMA
    inputs = [_in_hbm(a) for a in (*weights, *vectors, hid, lens, kc, vc)]
    return pl.pallas_call(
        _gather_kernel,
        out_shape=[pltpu.VMEM(size, BF16) for size in sizes],
        in_specs=[anywhere] * len(inputs),
        out_specs=[vmem] * len(sizes),
        scratch_shapes=[pltpu.VMEM(w.shape, BF16) for w in weights]
        + [pltpu.VMEM((4, weights[w].shape[0], QUARTER), BF16) for w in ROW_SHARED] + [
            pltpu.VMEM((TP, BLOCK, FF_PAD), BF16), pltpu.VMEM((5, 1, BLOCK), BF16), pltpu.VMEM(lens.shape, jnp.int32),
            pltpu.VMEM((2, 1, LANES), F32), pltpu.VMEM((TP * DP, 2, 1, LANES), F32), pltpu.VMEM(hid.shape, BF16),
            dma((11,)), dma((5,)), dma((7,)), dma((7, 4)), dma((7, 4)), dma((7, 4)), dma((7,)),
            dma((4, SPREAD_SENDS)), dma((4, SPREAD_RECVS)), dma, dma],
        compiler_params=pltpu.CompilerParams(collective_id=0, has_side_effects=True, vmem_limit_bytes=16 * MIB),
        cost_estimate=pl.CostEstimate(flops=2 * 10**10, bytes_accessed=MIB, transcendentals=0),
        name="gather",
    )(*inputs)


SLOTS = 8
BUFFERS = 3


def _attend_kernel(
    kc, vc, qt, kn, vn, lens, wq, wk, wv, wo, bq, bk, bv, ga, gm,
    ko, vo, out, oq, ok, ov, oo, obq, obk, obv, oga, ogm,
    stage, score, total, qf, sem, pass_sem,
):
    count = kc.shape[0] // SLOTS
    passing = [pltpu.make_async_copy(src, dst, pass_sem.at[i])
               for i, (src, dst) in enumerate(((wq, oq), (wk, ok), (wv, ov), (wo, oo)))]
    for copy in passing:
        copy.start()
    for src, dst in ((bq, obq), (bk, obk), (bv, obv), (ga, oga), (gm, ogm)):
        dst[...] = src[...].reshape(dst.shape)
    qf[...] = qt[...].astype(F32)
    lens_row = lens[...]
    lens_b = lens_row.astype(F32).astype(BF16)

    def put(dst, index, chunk):
        return pltpu.make_async_copy(stage.at[index], dst.at[pl.ds(chunk * SLOTS, SLOTS)], sem.at[index])

    def scores(chunk, index):
        for h in range(TP):
            query = qf[HEAD * h:HEAD * (h + 1)]
            fresh = kn[HEAD * h:HEAD * (h + 1)]
            parts = []
            for i in range(SLOTS):
                slot = chunk * SLOTS + i
                here = lens_b == slot.astype(F32).astype(BF16)
                keys = jnp.where(here, fresh, kc[slot, h])
                stage[index, i, h] = keys
                parts.append(jnp.sum(keys.astype(F32) * query, axis=0, keepdims=True))
            score[h, pl.ds(pl.multiple_of(chunk * SLOTS, SLOTS), SLOTS)] = jnp.concatenate(parts, axis=0)

    def values(chunk, index):
        for h in range(TP):
            fresh = vn[HEAD * h:HEAD * (h + 1)]
            weights = score[h, pl.ds(pl.multiple_of(chunk * SLOTS, SLOTS), SLOTS)]
            acc = total[HEAD * h:HEAD * (h + 1)]
            for i in range(SLOTS):
                slot = chunk * SLOTS + i
                here = lens_b == slot.astype(F32).astype(BF16)
                vals = jnp.where(here, fresh, vc[slot, h])
                stage[index, i, h] = vals
                acc = acc + vals.astype(F32) * weights[i:i + 1]
            total[HEAD * h:HEAD * (h + 1)] = acc

    def run(body, dst, first):
        @pl.loop(0, count)
        def _(chunk):
            index = (chunk + first) % BUFFERS

            @pl.when(chunk + first >= BUFFERS)
            def _():
                put(dst, index, 0).wait()

            body(chunk, index)
            put(dst, index, chunk).start()

    run(scores, ko, 0)
    visible = _iota((kc.shape[0], QUARTER), 0) <= lens_row
    for h in range(TP):
        raw = jnp.where(visible, score[h] * (HEAD ** -0.5), -1e30)
        top = jnp.max(raw, axis=0, keepdims=True)
        weight = jnp.exp(raw - top)
        score[h] = (weight / jnp.sum(weight, axis=0, keepdims=True)).astype(BF16).astype(F32)
    total[...] = jnp.zeros_like(total)
    run(values, vo, count)
    out[...] = total[...].T.astype(BF16)
    for index in range(BUFFERS):
        put(vo, index, 0).wait()
    for copy in passing:
        copy.wait()


def _attend(kc, vc, qt, kn, vn, lens, weights, vectors):
    hbm, vmem = pl.BlockSpec(memory_space=pltpu.HBM), pl.BlockSpec(memory_space=pltpu.VMEM)
    return pl.pallas_call(
        _attend_kernel,
        out_shape=[jax.ShapeDtypeStruct(kc.shape, BF16), jax.ShapeDtypeStruct(vc.shape, BF16),
                   jax.ShapeDtypeStruct((QUARTER, QUARTER), BF16)]
        + [jax.ShapeDtypeStruct(w.shape, BF16) for w in weights]
        + [jax.ShapeDtypeStruct((v.size,), BF16) for v in vectors],
        in_specs=[vmem] * 15,
        out_specs=[hbm, hbm, vmem] + [hbm] * 4 + [vmem] * 5,
        scratch_shapes=[pltpu.VMEM((BUFFERS, SLOTS) + kc.shape[1:], BF16), pltpu.VMEM((TP, kc.shape[0], QUARTER), F32),
                        pltpu.VMEM((QUARTER, QUARTER), F32), pltpu.VMEM((QUARTER, QUARTER), F32),
                        pltpu.SemaphoreType.DMA((BUFFERS,)), pltpu.SemaphoreType.DMA((4,))],
        compiler_params=pltpu.CompilerParams(vmem_limit_bytes=14 * MIB),
        cost_estimate=pl.CostEstimate(flops=10**10, bytes_accessed=32 * MIB, transcendentals=0),
        name="attend",
    )(kc, vc, qt, kn, vn, lens, *weights, *vectors)


ROOT = TP * WIDE_BLOCK
CHUNK = 32
CHUNKS = QUARTER // CHUNK
LAG = 2


class _LineSum:
    def __init__(self, part, inbox, mid, cross, send, recv):
        self.part, self.inbox, self.mid, self.cross, self.send, self.recv = part, inbox, mid, cross, send, recv
        z, dp = lax.axis_index("tp"), lax.axis_index("dp")
        self.pair, self.across, self.dp = z + 1 - 2 * (z % 2), 3 - z, dp
        self.inner = jnp.logical_and(z >= 1, z <= 2)

    def rows(self, k):
        return pl.ds(k * CHUNK, CHUNK)

    def to_pair(self, ref, k):
        return _remote(ref.at[self.rows(k)], self.inbox.at[self.rows(k)], self.send.at[0, k], self.recv.at[0, k],
                       self.pair, self.dp)

    def to_across(self, k):
        return _remote(self.mid.at[self.rows(k)], self.cross.at[self.rows(k)], self.send.at[1, k], self.recv.at[1, k],
                       self.across, self.dp)

    def push(self, k):
        @pl.when(jnp.logical_not(self.inner))
        def _():
            self.to_pair(self.part, k).start()

    def join(self, k):
        @pl.when(self.inner)
        def _():
            rows = self.rows(k)
            self.to_pair(self.part, k).wait_recv()
            self.mid[rows] = (self.part[rows].astype(F32) + self.inbox[rows].astype(F32)).astype(BF16)
            self.to_across(k).start()

    def finish(self, k):
        rows = self.rows(k)

        @pl.when(self.inner)
        def _():
            self.to_across(k).wait_recv()
            self.part[rows] = (self.mid[rows].astype(F32) + self.cross[rows].astype(F32)).astype(BF16)
            self.to_pair(self.part, k).start()

        @pl.when(jnp.logical_not(self.inner))
        def _():
            self.to_pair(self.part, k).wait_recv()
            self.to_pair(self.part, k).wait_send()
            self.part[rows] = self.inbox[rows]

    def drain(self):
        @pl.when(self.inner)
        def _():
            for k in range(CHUNKS):
                self.to_pair(self.part, k).wait_send()
                self.to_across(k).wait_send()


def _mlp_kernel(
    o, wo, hid, rg, ru, rd, gain,
    out, og, ou, od,
    part, inbox, mid, cross, part2, inbox2, mid2, cross2, x1, norm, down,
    send1, recv1, send2, recv2, sp_send, sp_recv,
):
    z, dp, core, col, cols, peers = _place()

    barrier = pltpu.get_barrier_semaphore()
    pair, across = z + 1 - 2 * (z % 2), 3 - z
    inner = jnp.logical_and(z >= 1, z <= 2)
    _signal(barrier, pair, dp)
    for peer in ("x", "y", "d"):
        _signal(barrier, z, peers[peer])

    @pl.when(inner)
    def _():
        _signal(barrier, across, dp)

    part[...] = _dot(o[...], wo[...], 1, 1).astype(BF16)

    def rows_spread(w, root, ref):
        return _Spread(
            z, dp, cols, peers, root,
            lambda column: ref.at[_rows(core * ROOT, ROOT), _lanes(column * QUARTER, QUARTER)],
            lambda column, half: ref.at[_rows(core * ROOT + 176 * half, 176), _lanes(column * QUARTER, QUARTER)],
            ref.at[_rows((1 - core) * ROOT, ROOT), :],
            sp_send.at[w], sp_recv.at[w])

    spreads = [rows_spread(0, rg, og), rows_spread(1, ru, ou)]
    spreads.append(_Spread(
        z, dp, cols, peers, rd,
        lambda column: down.at[_rows((2 * column + core) * LANES, LANES), :],
        lambda column, half: down.at[_rows((2 * column + core) * LANES + HEAD * half, HEAD), :],
        down.at[pl.ds(0, 512), :],
        sp_send.at[2], sp_recv.at[2]))
    og[_rows(core * ROOT, ROOT), _lanes(col * QUARTER, QUARTER)] = rg[...]
    ou[_rows(core * ROOT, ROOT), _lanes(col * QUARTER, QUARTER)] = ru[...]
    down[_rows(dp * LANES, LANES), :] = rd[...]

    @pl.when(inner)
    def _():
        pl.semaphore_wait(barrier, 5)

    @pl.when(jnp.logical_not(inner))
    def _():
        pl.semaphore_wait(barrier, 4)

    first = _LineSum(part, inbox, mid, cross, send1, recv1)
    for k in range(CHUNKS):
        first.push(k)
    spreads[0].first()
    spreads[1].first()
    for k in range(CHUNKS):
        first.join(k)
        if k >= LAG:
            first.finish(k - LAG)
        if k == 2:
            spreads[0].second()
            spreads[2].first()
        if k == 5:
            spreads[1].second()
    for k in range(CHUNKS - LAG, CHUNKS):
        first.finish(k)
    spreads[0].third()
    spreads[2].second()
    spreads[1].third()

    x1[...] = (hid[...].astype(F32) + part[...].astype(F32)).astype(BF16)
    norm[...] = _rms(x1[...], gain[...].astype(F32))

    spreads[2].third()
    for spread in spreads:
        spread.last()
    od[...] = down[...].T[0:FF]

    second = _LineSum(part2, inbox2, mid2, cross2, send2, recv2)
    for half in range(2):
        rows = pl.ds(LANES * half, LANES)
        gate = _dot(norm[rows], og[...], 1, 1).astype(BF16).astype(F32)
        up = _dot(norm[rows], ou[...], 1, 1).astype(BF16).astype(F32)
        gated = (jax.nn.silu(gate) * up).astype(BF16)
        part2[rows] = _dot(gated, od[...], 1, 0).astype(BF16)
        for k in range(CHUNKS // 2 * half, CHUNKS // 2 * (half + 1)):
            second.push(k)
    for k in range(CHUNKS):
        second.join(k)
        if k >= LAG:
            second.finish(k - LAG)
    for k in range(CHUNKS - LAG, CHUNKS):
        second.finish(k)
    out[...] = (x1[...].astype(F32) + part2[...].astype(F32)).astype(BF16)

    first.drain()
    second.drain()
    for spread in spreads:
        spread.drain()


def _mlp(o, wo, hid, rg, ru, rd, gain):
    vmem = pl.BlockSpec(memory_space=pltpu.VMEM)
    sizes = [(QUARTER, WIDTH), (FF, WIDTH), (FF, WIDTH), (FF, WIDTH)]
    dma = pltpu.SemaphoreType.DMA
    return pl.pallas_call(
        _mlp_kernel,
        out_shape=[pltpu.VMEM(size, BF16) for size in sizes],
        in_specs=[vmem] * 7,
        out_specs=[vmem] * 4,
        scratch_shapes=[pltpu.VMEM((QUARTER, WIDTH), BF16)] * 10 + [pltpu.VMEM((WIDTH, FF_PAD), BF16)] + [
            dma((2, CHUNKS))] * 4 + [dma((3, SPREAD_SENDS)), dma((3, SPREAD_RECVS))],
        compiler_params=pltpu.CompilerParams(collective_id=1, has_side_effects=True, vmem_limit_bytes=24 * MIB),
        cost_estimate=pl.CostEstimate(flops=2 * 10**10, bytes_accessed=MIB, transcendentals=0),
        name="mlp",
    )(o, wo, hid, rg, ru, rd, gain)


def _emit_kernel(*refs):
    count = len(refs) // 2
    copies = [pltpu.make_async_copy(refs[i], refs[count + i], refs[-1].at[i]) for i in range(count)]
    for copy in copies:
        copy.start()
    for copy in copies:
        copy.wait()


def _emit(*arrays):
    vmem, hbm = pl.BlockSpec(memory_space=pltpu.VMEM), pl.BlockSpec(memory_space=pltpu.HBM)
    return pl.pallas_call(
        _emit_kernel,
        out_shape=[jax.ShapeDtypeStruct(a.shape, a.dtype) for a in arrays],
        in_specs=[vmem] * len(arrays),
        out_specs=[hbm] * len(arrays),
        scratch_shapes=[pltpu.SemaphoreType.DMA((len(arrays),))],
        compiler_params=pltpu.CompilerParams(vmem_limit_bytes=4 * MIB),
        name="emit",
    )(*arrays)


def solution(mesh):
    def local_step(wq, bq, wk, bk, wv, bv, wo, wg, wu, wd, ga, gm, hid, k_cache, v_cache, lengths):
        lens = lengths.reshape(1, -1)
        vectors = [v.reshape(1, -1) for v in (bq, bk, bv, ga, gm)]
        kc, vc = jnp.transpose(k_cache, (1, 2, 3, 0)), jnp.transpose(v_cache, (1, 2, 3, 0))
        (gq, gk, gv, go, rd, rg, ru, qt, kt, vt, gbq, gbk, gbv, gga, ggm, hid_v, kc_v, vc_v) = _gather(
            (wq, wk, wv, wo, wd, wg, wu), vectors, hid, lens, kc, vc)
        ko, vo, o, oq, ok, ov, oo, obq, obk, obv, oga, ogm = _attend(
            kc_v, vc_v, qt, kt, vt, lens, (gq, gk, gv, go), (gbq, gbk, gbv, gga, ggm))
        out, og, ou, od = _emit(*_mlp(o, go, hid_v, rg, ru, rd, ggm))
        return (oq, obq, ok, obk, ov, obv, oo, og, ou, od.T, oga, ogm, out,
                jnp.transpose(ko, (3, 0, 1, 2)), jnp.transpose(vo, (3, 0, 1, 2)))

    row_spec = P(("dp", "tp"), None)
    flat_spec = P(("dp", "tp"))
    cache_spec = P("dp", None, "tp", None)
    in_specs = (row_spec, flat_spec, row_spec, flat_spec, row_spec, flat_spec, row_spec, row_spec, row_spec, row_spec,
                flat_spec, flat_spec, P("dp", None), cache_spec, cache_spec, P("dp"))
    out_specs = (P("tp", None), P("tp"), P("tp", None), P("tp"), P("tp", None), P("tp"), P(None, "tp"), P("tp", None),
                 P("tp", None), P(None, "tp"), P(None), P(None), P("dp", None), cache_spec, cache_spec)
    return jax.shard_map(local_step, mesh=mesh, in_specs=in_specs, out_specs=out_specs, check_vma=False)
```

```python
import functools
import math

import jax
import jax.numpy as jnp
from jax import lax
from jax.experimental import pallas as pl
from jax.experimental.pallas import tpu as pltpu
from jax.sharding import PartitionSpec as P

EPS = 1e-6
THETA = 1000000.0
MESH = pl.DeviceIdType.MESH
BF16, F32 = jnp.bfloat16, jnp.float32
TP, DP = 4, 8
PEERS = TP * DP - 1
HEAD, HALF = 64, 32
WIDTH, QUARTER, LANES = 1024, 256, 128
BLOCK, WIDE_BLOCK = 32, 88
FF, FF_PAD = 704, 768
MIB = 2**20


def _place():
    z, dp = lax.axis_index("tp"), lax.axis_index("dp")
    core, col = dp % 2, dp // 2
    x, y = col % 2, col // 2
    cols = (col, col + 1 - 2 * x, col + 2 - 4 * y, 3 - col)
    peers = {"x": dp + 2 - 4 * x, "y": dp + 4 - 8 * y, "d": dp + 1 - 2 * core}
    return z, dp, core, col, cols, peers


def _remote(src, dst, send, recv, tp, dp):
    return pltpu.make_async_remote_copy(
        src_ref=src, dst_ref=dst, send_sem=send, recv_sem=recv, device_id={"tp": tp, "dp": dp}, device_id_type=MESH
    )


def _rows(start, size):
    return pl.ds(pl.multiple_of(start, 8), size)


def _lanes(start, size):
    return pl.ds(pl.multiple_of(start, 128), size)


def _signal(sem, tp, dp):
    pl.semaphore_signal(sem, inc=1, device_id={"tp": tp, "dp": dp}, device_id_type=MESH)


def _dot(a, b, ca, cb):
    return lax.dot_general(a, b, (((ca,), (cb,)), ((), ())), preferred_element_type=F32)


def _iota(shape, axis):
    return lax.broadcasted_iota(jnp.int32, shape, axis)


def _sublane(shape):
    return _iota(shape, 0)


def _lane(shape):
    return _iota(shape, 1)


def _in_hbm(array):
    return pltpu.with_memory_space_constraint(array, pltpu.HBM)


def _rms(act, gain_row):
    act = act.astype(F32)
    inv = lax.rsqrt(jnp.mean(act * act, axis=-1, keepdims=True) + EPS)
    return (act * inv * gain_row).astype(BF16)


class _Spread:
    def __init__(self, tp, dp, cols, peers, src_own, region, halves, total, send, recv):
        self.tp, self.cols, self.peers = tp, cols, peers
        self.src_own, self.region, self.halves, self.total = src_own, region, halves, total
        self.send, self.recv = send, recv
        self.sent = []

    def _go(self, src, dst, peer, recv_index):
        copy = _remote(src, dst, self.send.at[len(self.sent)], self.recv.at[recv_index], self.tp, self.peers[peer])
        copy.start()
        self.sent.append(copy)

    def _got(self, ref, recv_index):
        _remote(ref, ref, self.send.at[0], self.recv.at[recv_index], self.tp, self.peers["x"]).wait_recv()

    def first(self):
        own = self.region(self.cols[0])
        self._go(self.src_own, own, "x", 0)
        self._go(self.src_own, own, "y", 1)
        self._go(self.src_own, own, "d", 4)

    def second(self):
        at_x, at_y = self.region(self.cols[1]), self.region(self.cols[2])
        self._got(at_x, 0)
        upper = self.halves(self.cols[1], 0)
        self._go(upper, upper, "y", 2)
        self._go(at_x, at_x, "d", 4)
        self._got(at_y, 1)
        lower = self.halves(self.cols[2], 1)
        self._go(lower, lower, "x", 3)
        self._go(at_y, at_y, "d", 4)

    def third(self):
        upper, lower = self.halves(self.cols[3], 0), self.halves(self.cols[3], 1)
        self._got(upper, 2)
        self._go(upper, upper, "d", 4)
        self._got(lower, 3)
        self._go(lower, lower, "d", 4)

    def last(self):
        self._got(self.total, 4)

    def drain(self):
        for copy in self.sent:
            copy.wait_send()


SPREAD_SENDS, SPREAD_RECVS = 9, 5
Q, K, V, OUT, DOWN, GATE, UP = range(7)
ROW_SHARED = (Q, K, V, GATE, UP)
SLOTS = 8
CHUNK = 32
CHUNKS = QUARTER // CHUNK
BLOCK_CHUNKS = 2
LAG = 2


class _LineSum:
    def __init__(self, part, inbox, mid, cross, send, recv, use):
        self.part, self.inbox, self.mid, self.cross, self.send, self.recv = part, inbox, mid, cross, send, recv
        z, dp = lax.axis_index("tp"), lax.axis_index("dp")
        self.pair, self.across, self.dp = z + 1 - 2 * (z % 2), TP - 1 - z, dp
        self.inner = jnp.logical_and(z >= 1, z <= 2)
        self.outer = jnp.logical_not(self.inner)
        self.use = use

    def rows(self, k):
        return pl.ds(k * CHUNK, CHUNK)

    def to_pair(self, k):
        return _remote(self.part.at[self.rows(k)], self.inbox.at[self.rows(k)], self.send.at[0, k],
                       self.recv.at[0, k], self.pair, self.dp)

    def to_across(self, k):
        return _remote(self.mid.at[self.rows(k)], self.cross.at[self.rows(k)], self.send.at[1, k], self.recv.at[1, k],
                       self.across, self.dp)

    def push(self, k):
        @pl.when(self.outer)
        def _():
            self.to_pair(k).start()

    def join(self, k):
        @pl.when(self.inner)
        def _():
            rows = self.rows(k)
            self.to_pair(k).wait_recv()
            self.mid[rows] = (self.part[rows].astype(F32) + self.inbox[rows].astype(F32)).astype(BF16)
            self.to_across(k).start()

    def finish(self, k):
        rows = self.rows(k)

        @pl.when(self.inner)
        def _():
            self.to_across(k).wait_recv()
            total = (self.mid[rows].astype(F32) + self.cross[rows].astype(F32)).astype(BF16)
            self.part[rows] = total
            self.to_pair(k).start()
            self.use(rows, total)

        @pl.when(self.outer)
        def _():
            self.to_pair(k).wait_recv()
            self.use(rows, self.inbox[rows])

    def drain(self):
        for k in range(CHUNKS):
            self.to_pair(k).wait_send()

        @pl.when(self.inner)
        def _():
            for k in range(CHUNKS):
                self.to_across(k).wait_send()


def _step_kernel(
    wq, wk, wv, wo, wd, wg, wu, bq, bk, bv, ga, gm, hid_hbm, lens_hbm, kc_hbm, vc_hbm,
    oq, ok, ov, oo, od, og, ou, kt, vt, obq, obk, obv, oga, ogm, kc, vc, lens, out,
    sq, sk, sv, so, sd, sg, su, tq, tk, tv, tg, tu, dcut, vecs, hid, aux, board, act, qt,
    score, total, attended, part, inbox, mid, cross, part2, inbox2, mid2, cross2, x1,
    load_sem, vec_sem, own_sem, s0_send, s0_recv, s1_send, s1_recv, sp_send, sp_recv, aux_send, aux_recv,
    send1, recv1, send2, recv2,
):
    z, dp, core, col, cols, peers = _place()
    device = dp * TP + z
    own_here = z == col
    away = jnp.logical_not(own_here)
    at_peer = (dp, peers["x"], peers["y"], 2 * cols[3] + core)
    hbm = (wq, wk, wv, wo, wd, wg, wu)
    source = (sq, sk, sv, so, sd, sg, su)
    share = (oq, ok, ov, oo, od, og, ou)
    staged = {Q: tq, K: tk, V: tv, GATE: tg, UP: tu}

    loads = [pltpu.make_async_copy(src, dst, load_sem.at[i]) for i, (src, dst) in enumerate(
        zip(hbm + (hid_hbm, lens_hbm, kc_hbm, vc_hbm), source + (hid, lens, kc, vc)))]
    small = [pltpu.make_async_copy(src, vecs.at[i], vec_sem.at[i]) for i, src in enumerate((bq, bk, bv, ga, gm))]
    for copy in loads[:UP + 1] + small + loads[UP + 1:]:
        copy.start()

    barrier = pltpu.get_barrier_semaphore()

    @pl.loop(1, TP * DP)
    def _(k):
        other = (device + k) % (TP * DP)
        _signal(barrier, other % TP, other // TP)

    for copy in small:
        copy.wait()
    spots = [(_lane((BLOCK, LANES)) == _sublane((BLOCK, LANES)) + BLOCK * r).astype(BF16) for r in range(TP)]
    aux[0] = sum(_dot(vecs[r], spot, 1, 0) for r, spot in enumerate(spots))
    aux[1] = _dot(vecs[TP], spots[0], 1, 0)
    board[pl.ds(device, 1)] = aux[...].reshape(1, 2, 1, LANES)
    for w in (Q, K, V, OUT, GATE, UP):
        loads[w].wait()

    pl.semaphore_wait(barrier, PEERS)

    sent = []
    guarded = []

    def lanes_of(column):
        return _lanes(column * QUARTER, QUARTER)

    def root(w, plane_row):
        rows = source[w].shape[0]
        return lambda column: share[w].at[_rows((core * TP + plane_row) * rows, rows), lanes_of(column)]

    def own_piece(w):
        return pltpu.make_async_copy(hbm[w].at[:, lanes_of(col)], root(w, z)(col), own_sem.at[w])

    def scatter(w):
        for m in (1, 2, 3):
            src = source[w].at[:, lanes_of(cols[m])]
            sems = s0_send.at[w, m], s0_recv.at[w, m], z, at_peer[m]
            landing = _remote(src, root(w, z)(cols[m]), *sems)
            passing = _remote(src, staged[w].at[m], *sems)

            @pl.when(own_here)
            def _():
                landing.start()

            @pl.when(away)
            def _():
                passing.start()
            sent.append(passing)

        @pl.when(own_here)
        def _():
            own_piece(w).start()

    def forward(w):
        for m in range(4):
            piece = source[w].at[:, lanes_of(col)] if m == 0 else staged[w].at[m]
            copy = _remote(piece, root(w, z)(col), s1_send.at[w, m], s1_recv.at[w], cols[m], dp)
            if m:
                _remote(staged[w].at[m], staged[w].at[m], s0_send.at[w, m], s0_recv.at[w, m], z, dp).wait_recv()
            elsewhere = cols[m] != z

            @pl.when(elsewhere)
            def _():
                copy.start()
            guarded.append((elsewhere, copy))

    def columns(w, piece, dst):
        for m in (1, 2, 3):
            plane = (z + m) % TP
            copy = _remote(piece(plane), dst, s1_send.at[w, m], s1_recv.at[w], plane, dp)
            copy.start()
            sent.append(copy)

    def got_root(w):
        rows = source[w].shape[0]
        width = QUARTER if w in ROW_SHARED else share[w].shape[1]
        three = share[w].at[pl.ds(0, 3 * rows), pl.ds(0, width)]
        _remote(three, three, s1_send.at[w, 1], s1_recv.at[w], z, peers["x"]).wait_recv()
        if w in ROW_SHARED:
            @pl.when(own_here)
            def _():
                own_piece(w).wait()

    def rows_spread(w, index):
        ref, size = share[w], TP * source[w].shape[0]
        return _Spread(
            z, dp, cols, peers,
            ref.at[_rows(core * size, size), lanes_of(col)],
            lambda column: ref.at[_rows(core * size, size), lanes_of(column)],
            lambda column, half: ref.at[_rows(core * size + size // 2 * half, size // 2), lanes_of(column)],
            ref.at[_rows((1 - core) * size, size), :],
            sp_send.at[index], sp_recv.at[index])

    def columns_spread(w, index):
        ref = share[w]
        return _Spread(
            z, dp, cols, peers,
            ref.at[_rows(dp * LANES, LANES), :],
            lambda column: ref.at[_rows((2 * column + core) * LANES, LANES), :],
            lambda column, half: ref.at[_rows((2 * column + core) * LANES + HEAD * half, HEAD), :],
            ref.at[pl.ds(0, WIDTH // 2), :],
            sp_send.at[index], sp_recv.at[index])

    spreads = [(rows_spread if w in ROW_SHARED else columns_spread)(w, w) for w in range(7)]

    for w in (Q, K, V):
        scatter(w)
    out_rows = oo.at[_rows(dp * LANES + z * BLOCK, BLOCK), :]
    out_own = pltpu.make_async_copy(wo.at[:, lanes_of(z)], out_rows, own_sem.at[OUT])
    out_own.start()
    columns(OUT, lambda plane: so.at[:, lanes_of(plane)], out_rows)

    def announce(k):
        other = (device + k) % (TP * DP)
        return _remote(aux, board.at[device], aux_send, aux_recv, other % TP, other // TP)

    @pl.loop(1, TP * DP)
    def _(k):
        announce(k).start()

    for w in (GATE, UP):
        scatter(w)
    for w in (Q, K, V):
        forward(w)
    for w in (GATE, UP):
        forward(w)
    loads[DOWN].wait()
    for t in range(TP):
        dcut[t, :, :FF] = sd[:, FF * t:FF * (t + 1)]
        dcut[t, :, FF:] = jnp.zeros((BLOCK, FF_PAD - FF), BF16)
    down_rows = od.at[_rows(dp * LANES + z * BLOCK, BLOCK), :]
    down_rows[...] = dcut[z]
    columns(DOWN, lambda plane: dcut.at[plane], down_rows)

    landed = board.at[pl.ds(0, PEERS)]
    _remote(landed, landed, aux_send, aux_recv, z, peers["x"]).wait_recv()
    sub = _sublane((BLOCK, LANES))
    first, second = jnp.zeros((BLOCK, LANES), F32), jnp.zeros((BLOCK, LANES), F32)
    for i in range(TP * DP):
        first = jnp.where(sub == i, board[i, 0], first)
        second = jnp.where(sub == i, board[i, 1], second)
    first, second = first.astype(BF16), second.astype(BF16)

    def spread_row(table, offset, count, keep):
        width = count * BLOCK
        spot = (_sublane((LANES, width)) == _lane((LANES, width)) % BLOCK + offset).astype(BF16)
        wide = _dot(table, spot, 1, 0)
        mine = _sublane((BLOCK, width)) == keep + _lane((BLOCK, width)) // BLOCK
        return jnp.sum(jnp.where(mine, wide, 0.0), axis=0, keepdims=True)

    gain_row = spread_row(first, 3 * BLOCK, TP * DP, 0)
    gain_mlp = spread_row(second, 0, TP * DP, 0)
    oga[...] = gain_row.astype(BF16)
    ogm[...] = gain_mlp.astype(BF16)
    for r, ref in enumerate((obq, obk, obv)):
        ref[...] = spread_row(first, BLOCK * r, DP, DP * z).astype(BF16)

    def bias_column(r):
        tall_shape = (QUARTER, BLOCK)
        pick = (_lane(tall_shape) == DP * z + _sublane(tall_shape) // BLOCK).astype(BF16)
        tall = _dot(pick, first, 1, 0)
        mine = _lane(tall.shape) == BLOCK * r + _sublane(tall.shape) % BLOCK
        return jnp.sum(jnp.where(mine, tall, 0.0), axis=1, keepdims=True)

    for copy in loads[UP + 1:UP + 3]:
        copy.wait()
    act[...] = _rms(hid[...], gain_row)

    lens_row = lens[...]
    inv_freq = jnp.exp(_sublane((HALF, QUARTER)).astype(F32) * (-math.log(THETA) / HALF))
    angle = lens_row.astype(F32) * inv_freq
    cosine, sine = jnp.cos(angle), jnp.sin(angle)

    for w in (Q, K, V):
        got_root(w)
        spreads[w].first()
    out_own.wait()
    got_root(OUT)
    spreads[OUT].first()
    spreads[Q].second()
    spreads[K].second()
    spreads[V].second()
    spreads[Q].third()
    spreads[OUT].second()
    spreads[K].third()
    spreads[V].third()
    got_root(GATE)
    spreads[GATE].first()

    def project(weight, r):
        return (_dot(weight[...], act[...], 1, 1) + bias_column(r)).astype(BF16)

    def rotate(vec, out):
        vec = vec.astype(F32)
        for h in range(TP):
            base = HEAD * h
            lo, hi = vec[base:base + HALF], vec[base + HALF:base + HEAD]
            out[base:base + HALF] = (lo * cosine - hi * sine).astype(BF16).astype(out.dtype)
            out[base + HALF:base + HEAD] = (hi * cosine + lo * sine).astype(BF16).astype(out.dtype)

    spreads[Q].last()
    rotate(project(oq, Q), qt)
    spreads[K].last()
    rotate(project(ok, K), kt)
    spreads[V].last()
    vt[...] = project(ov, V)
    for copy in loads[UP + 3:]:
        copy.wait()
    spreads[OUT].third()

    def heads(h):
        return slice(HEAD * h, HEAD * (h + 1))

    def chunk_rows(chunk):
        return pl.ds(pl.multiple_of(chunk * SLOTS, SLOTS), SLOTS)

    def scores(start, stop):
        @pl.loop(start, stop)
        def _(chunk):
            for h in range(TP):
                query = qt[heads(h)]
                score[h, chunk_rows(chunk)] = jnp.concatenate([
                    jnp.sum(kc[chunk * SLOTS + i, h].astype(F32) * query, axis=0, keepdims=True)
                    for i in range(SLOTS)], axis=0)

    def values(start, stop):
        @pl.loop(start, stop)
        def _(chunk):
            for h in range(TP):
                weights = score[h, chunk_rows(chunk)]
                acc = total[heads(h)]
                for i in range(SLOTS):
                    acc = acc + vc[chunk * SLOTS + i, h].astype(F32) * weights[i:i + 1]
                total[heads(h)] = acc

    count = kc.shape[0] // SLOTS
    scores(0, count // 2)
    got_root(UP)
    spreads[UP].first()
    scores(count // 2, count)
    spreads[GATE].second()
    slot = _sublane((kc.shape[0], QUARTER))
    for h in range(TP):
        fresh = jnp.sum(kt[heads(h)].astype(F32) * qt[heads(h)], axis=0, keepdims=True)
        raw = jnp.where(slot == lens_row, fresh, score[h]) * (HEAD ** -0.5)
        raw = jnp.where(slot <= lens_row, raw, -1e30)
        weight = jnp.exp(raw - jnp.max(raw, axis=0, keepdims=True))
        weight = (weight / jnp.sum(weight, axis=0, keepdims=True)).astype(BF16).astype(F32)
        newest = jnp.sum(jnp.where(slot == lens_row, weight, 0.0), axis=0, keepdims=True)
        score[h] = jnp.where(slot == lens_row, 0.0, weight)
        total[heads(h)] = vt[heads(h)].astype(F32) * newest
    values(0, count // 2)
    got_root(DOWN)
    spreads[DOWN].first()
    values(count // 2, count)
    attended[...] = total[...].T.astype(BF16)
    spreads[UP].second()
    spreads[OUT].last()

    def after_first(rows, total_rows):
        x1[rows] = (hid[rows].astype(F32) + total_rows.astype(F32)).astype(BF16)

    def after_second(rows, total_rows):
        out[rows] = (x1[rows].astype(F32) + total_rows.astype(F32)).astype(BF16)

    line1 = _LineSum(part, inbox, mid, cross, send1, recv1, after_first)
    line2 = _LineSum(part2, inbox2, mid2, cross2, send2, recv2, after_second)

    for half in range(2):
        rows = pl.ds(LANES * half, LANES)
        part[rows] = _dot(attended[rows], oo[...], 1, 1).astype(BF16)
        for k in range(CHUNKS // 2 * half, CHUNKS // 2 * (half + 1)):
            line1.push(k)
    spreads[GATE].third()
    spreads[DOWN].second()
    spreads[UP].third()

    def mlp(block):
        size = BLOCK_CHUNKS * CHUNK
        rows = pl.ds(block * size, size)
        norm = _rms(x1[rows], gain_mlp)
        gate = _dot(norm, og[...], 1, 1).astype(BF16).astype(F32)
        up = _dot(norm, ou[...], 1, 1).astype(BF16).astype(F32)
        gated = (jax.nn.silu(gate) * up).astype(BF16)
        part2[rows] = _dot(gated, od[:, :FF], 1, 1).astype(BF16)
        for k in range(block * BLOCK_CHUNKS, (block + 1) * BLOCK_CHUNKS):
            line2.push(k)

    def finish_first(k):
        line1.finish(k)
        if k == 1:
            for w in (GATE, UP, DOWN):
                spreads[w].last()
        if (k + 1) % BLOCK_CHUNKS == 0:
            mlp(k // BLOCK_CHUNKS)

    for k in range(CHUNKS):
        line1.join(k)
        if k == LAG:
            spreads[DOWN].third()
        if k >= LAG:
            finish_first(k - LAG)
    for k in range(CHUNKS - LAG, CHUNKS):
        finish_first(k)
    for k in range(CHUNKS):
        line2.join(k)
        if k >= LAG:
            line2.finish(k - LAG)
    for k in range(CHUNKS - LAG, CHUNKS):
        line2.finish(k)

    line1.drain()
    line2.drain()
    for copy in sent:
        copy.wait_send()
    for elsewhere, copy in guarded:
        @pl.when(elsewhere)
        def _():
            copy.wait_send()
    for spread in spreads:
        spread.drain()
    _remote(landed, landed, aux_send, aux_recv, z, peers["x"]).wait_send()


def _step(weights, vectors, hid, lens, kc, vc):
    vmem = pl.BlockSpec(memory_space=pltpu.VMEM)
    anywhere = pl.BlockSpec(memory_space=pltpu.HBM)
    square = (QUARTER, QUARTER)
    sizes = [(QUARTER, WIDTH)] * 3 + [(WIDTH, QUARTER), (WIDTH, FF_PAD)] + [(FF, WIDTH)] * 2
    sizes += [square] * 2 + [(1, QUARTER)] * 3 + [(1, WIDTH)] * 2 + [kc.shape, vc.shape]
    outs = [pltpu.VMEM(size, BF16) for size in sizes] + [pltpu.VMEM(lens.shape, lens.dtype), pltpu.VMEM(hid.shape, BF16)]
    dma = pltpu.SemaphoreType.DMA
    inputs = [_in_hbm(a) for a in (*weights, *vectors, hid, lens, kc, vc)]
    rows = pltpu.VMEM(hid.shape, BF16)
    return pl.pallas_call(
        _step_kernel,
        out_shape=outs,
        in_specs=[anywhere] * len(inputs),
        out_specs=[vmem] * len(outs),
        scratch_shapes=[pltpu.VMEM(w.shape, BF16) for w in weights]
        + [pltpu.VMEM((4, weights[w].shape[0], QUARTER), BF16) for w in ROW_SHARED] + [
            pltpu.VMEM((TP, BLOCK, FF_PAD), BF16), pltpu.VMEM((5, 1, BLOCK), BF16), rows,
            pltpu.VMEM((2, 1, LANES), F32), pltpu.VMEM((TP * DP, 2, 1, LANES), F32), rows, pltpu.VMEM(square, F32),
            pltpu.VMEM((TP, kc.shape[0], QUARTER), F32), pltpu.VMEM(square, F32), pltpu.VMEM(square, BF16)]
        + [rows] * 9 + [
            dma((11,)), dma((5,)), dma((7,)), dma((7, 4)), dma((7, 4)), dma((7, 4)), dma((7,)),
            dma((7, SPREAD_SENDS)), dma((7, SPREAD_RECVS)), dma, dma] + [dma((2, CHUNKS))] * 4,
        compiler_params=pltpu.CompilerParams(collective_id=0, has_side_effects=True, vmem_limit_bytes=24 * MIB),
        cost_estimate=pl.CostEstimate(flops=2 * 10**10, bytes_accessed=MIB, transcendentals=0),
        name="step",
    )(*inputs)


BUFFERS = 4


def _emit_kernel(*refs):
    kc, vc, kn, vn, lens, down = refs[:6]
    plain = refs[6:13]
    vectors = refs[13:18]
    ko, vo, od = refs[18:21]
    plain_out = refs[21:28]
    vectors_out = refs[28:33]
    stage, turned, sem, pass_sem, down_sem = refs[33:]

    passing = [pltpu.make_async_copy(src, dst, pass_sem.at[i]) for i, (src, dst) in enumerate(zip(plain, plain_out))]
    for copy in passing:
        copy.start()
    for src, dst in zip(vectors, vectors_out):
        dst[...] = src[...].reshape(dst.shape)

    lens_b = lens[...].astype(F32).astype(BF16)
    count = kc.shape[0] // SLOTS

    def put(dst, index, chunk):
        return pltpu.make_async_copy(stage.at[index], dst.at[pl.ds(chunk * SLOTS, SLOTS)], sem.at[index])

    def update(old, new, dst, first):
        @pl.loop(0, count)
        def _(chunk):
            index = (chunk + first) % BUFFERS

            @pl.when(chunk + first >= BUFFERS)
            def _():
                put(dst, index, 0).wait()

            for i in range(SLOTS):
                slot = chunk * SLOTS + i
                here = lens_b == slot.astype(F32).astype(BF16)
                for h in range(TP):
                    stage[index, i, h] = jnp.where(here, new[HEAD * h:HEAD * (h + 1)], old[slot, h])
            put(dst, index, chunk).start()

    update(kc, kn, ko, 0)
    turned[...] = down[...].T
    turn = pltpu.make_async_copy(turned.at[pl.ds(0, FF)], od, down_sem)
    turn.start()
    update(vc, vn, vo, count)
    for index in range(BUFFERS):
        put(vo, index, 0).wait()
    for copy in passing + [turn]:
        copy.wait()


def _emit(kc, vc, kn, vn, lens, down, plain, vectors):
    vmem, hbm = pl.BlockSpec(memory_space=pltpu.VMEM), pl.BlockSpec(memory_space=pltpu.HBM)
    shapes = [kc.shape, vc.shape, (FF, WIDTH)] + [a.shape for a in plain] + [(v.size,) for v in vectors]
    dma = pltpu.SemaphoreType.DMA
    return pl.pallas_call(
        _emit_kernel,
        out_shape=[jax.ShapeDtypeStruct(shape, BF16) for shape in shapes],
        in_specs=[vmem] * (6 + len(plain) + len(vectors)),
        out_specs=[hbm] * (3 + len(plain)) + [vmem] * len(vectors),
        scratch_shapes=[pltpu.VMEM((BUFFERS, SLOTS) + kc.shape[1:], BF16), pltpu.VMEM((FF_PAD, WIDTH), BF16),
                        dma((BUFFERS,)), dma((len(plain),)), dma],
        compiler_params=pltpu.CompilerParams(vmem_limit_bytes=12 * MIB),
        cost_estimate=pl.CostEstimate(flops=10**9, bytes_accessed=24 * MIB, transcendentals=0),
        name="emit",
    )(kc, vc, kn, vn, lens, down, *plain, *vectors)


def solution(mesh):
    def local_step(wq, bq, wk, bk, wv, bv, wo, wg, wu, wd, ga, gm, hid, k_cache, v_cache, lengths):
        vectors = [v.reshape(1, -1) for v in (bq, bk, bv, ga, gm)]
        kc, vc = jnp.transpose(k_cache, (1, 2, 3, 0)), jnp.transpose(v_cache, (1, 2, 3, 0))
        (gq, gk, gv, go, gd, gg, gu, kt, vt, gbq, gbk, gbv, gga, ggm, kc_v, vc_v, lens_v, out_v) = _step(
            (wq, wk, wv, wo, wd, wg, wu), vectors, hid, lengths.reshape(1, -1), kc, vc)
        ko, vo, od, oq, ok, ov, oo, og, ou, out, obq, obk, obv, oga, ogm = _emit(
            kc_v, vc_v, kt, vt, lens_v, gd, (gq, gk, gv, go, gg, gu, out_v), (gbq, gbk, gbv, gga, ggm))
        return (oq, obq, ok, obk, ov, obv, oo, og, ou, od.T, oga, ogm, out,
                jnp.transpose(ko, (3, 0, 1, 2)), jnp.transpose(vo, (3, 0, 1, 2)))

    row_spec = P(("dp", "tp"), None)
    flat_spec = P(("dp", "tp"))
    cache_spec = P("dp", None, "tp", None)
    in_specs = (row_spec, flat_spec, row_spec, flat_spec, row_spec, flat_spec, row_spec, row_spec, row_spec, row_spec,
                flat_spec, flat_spec, P("dp", None), cache_spec, cache_spec, P("dp"))
    out_specs = (P("tp", None), P("tp"), P("tp", None), P("tp"), P("tp", None), P("tp"), P(None, "tp"), P("tp", None),
                 P("tp", None), P(None, "tp"), P(None), P(None), P("dp", None), cache_spec, cache_spec)
    return jax.shard_map(local_step, mesh=mesh, in_specs=in_specs, out_specs=out_specs, check_vma=False)
```

```python
import math

import jax
import jax.numpy as jnp
from jax import lax
from jax.experimental import pallas as pl
from jax.experimental.pallas import tpu as pltpu
from jax.sharding import PartitionSpec as P

EPS = 1e-6
THETA = 1000000.0
MESH = pl.DeviceIdType.MESH
BF16, F32 = jnp.bfloat16, jnp.float32
TP, DP = 4, 8
HEAD, HALF = 64, 32
WIDTH, QUARTER, LANES = 1024, 256, 128
BLOCK, WIDE_BLOCK = 32, 88
FF, FF_PAD = 704, 768
MIB = 2**20


def _place():
    z, dp = lax.axis_index("tp"), lax.axis_index("dp")
    core, col = dp % 2, dp // 2
    x, y = col % 2, col // 2
    cols = (col, col + 1 - 2 * x, col + 2 - 4 * y, 3 - col)
    peers = {"x": dp + 2 - 4 * x, "y": dp + 4 - 8 * y, "d": dp + 1 - 2 * core}
    return z, dp, core, col, cols, peers


def _remote(src, dst, send, recv, tp, dp):
    return pltpu.make_async_remote_copy(
        src_ref=src, dst_ref=dst, send_sem=send, recv_sem=recv, device_id={"tp": tp, "dp": dp}, device_id_type=MESH
    )


def _rows(start, size):
    return pl.ds(pl.multiple_of(start, 8), size)


def _lanes(start, size):
    return pl.ds(pl.multiple_of(start, 128), size)


def _signal(sem, tp, dp):
    pl.semaphore_signal(sem, inc=1, device_id={"tp": tp, "dp": dp}, device_id_type=MESH)


def _dot(a, b, ca, cb):
    return lax.dot_general(a, b, (((ca,), (cb,)), ((), ())), preferred_element_type=F32)


def _iota(shape, axis):
    return lax.broadcasted_iota(jnp.int32, shape, axis)


def _sublane(shape):
    return _iota(shape, 0)


def _lane(shape):
    return _iota(shape, 1)


def _in_hbm(array):
    return pltpu.with_memory_space_constraint(array, pltpu.HBM)


def _rms(act, gain_row):
    act = act.astype(F32)
    inv = lax.rsqrt(jnp.mean(act * act, axis=-1, keepdims=True) + EPS)
    return (act * inv * gain_row).astype(BF16)


class _Spread:
    def __init__(self, tp, dp, cols, peers, src_own, region, halves, total, send, recv):
        self.tp, self.cols, self.peers = tp, cols, peers
        self.src_own, self.region, self.halves, self.total = src_own, region, halves, total
        self.send, self.recv = send, recv
        self.sent = []

    def _go(self, src, dst, peer, recv_index):
        copy = _remote(src, dst, self.send.at[len(self.sent)], self.recv.at[recv_index], self.tp, self.peers[peer])
        copy.start()
        self.sent.append(copy)

    def _got(self, ref, recv_index):
        _remote(ref, ref, self.send.at[0], self.recv.at[recv_index], self.tp, self.peers["x"]).wait_recv()

    def first(self):
        own = self.region(self.cols[0])
        self._go(self.src_own, own, "x", 0)
        self._go(self.src_own, own, "y", 1)
        self._go(self.src_own, own, "d", 4)

    def second(self):
        at_x, at_y = self.region(self.cols[1]), self.region(self.cols[2])
        self._got(at_x, 0)
        upper = self.halves(self.cols[1], 0)
        self._go(upper, upper, "y", 2)
        self._go(at_x, at_x, "d", 4)
        self._got(at_y, 1)
        lower = self.halves(self.cols[2], 1)
        self._go(lower, lower, "x", 3)
        self._go(at_y, at_y, "d", 4)

    def third(self):
        upper, lower = self.halves(self.cols[3], 0), self.halves(self.cols[3], 1)
        self._got(upper, 2)
        self._go(upper, upper, "d", 4)
        self._got(lower, 3)
        self._go(lower, lower, "d", 4)

    def last(self):
        self._got(self.total, 4)

    def drain(self):
        for copy in self.sent:
            copy.wait_send()


SPREAD_SENDS, SPREAD_RECVS = 9, 5
Q, K, V, OUT, DOWN, GATE, UP = range(7)
ROW_SHARED = (Q, K, V, GATE, UP)
SLOTS = 8
CHUNK = 32
CHUNKS = QUARTER // CHUNK
BLOCK_CHUNKS = 2
LAG = 2


class _LineSum:
    def __init__(self, part, inbox, mid, cross, send, recv, use):
        self.part, self.inbox, self.mid, self.cross, self.send, self.recv = part, inbox, mid, cross, send, recv
        z, dp = lax.axis_index("tp"), lax.axis_index("dp")
        self.pair, self.across, self.dp = z + 1 - 2 * (z % 2), TP - 1 - z, dp
        self.inner = jnp.logical_and(z >= 1, z <= 2)
        self.outer = jnp.logical_not(self.inner)
        self.use = use

    def rows(self, k):
        return pl.ds(k * CHUNK, CHUNK)

    def to_pair(self, k):
        return _remote(self.part.at[self.rows(k)], self.inbox.at[self.rows(k)], self.send.at[0, k],
                       self.recv.at[0, k], self.pair, self.dp)

    def to_across(self, k):
        return _remote(self.mid.at[self.rows(k)], self.cross.at[self.rows(k)], self.send.at[1, k], self.recv.at[1, k],
                       self.across, self.dp)

    def push(self, k):
        @pl.when(self.outer)
        def _():
            self.to_pair(k).start()

    def join(self, k):
        @pl.when(self.inner)
        def _():
            rows = self.rows(k)
            self.to_pair(k).wait_recv()
            self.mid[rows] = (self.part[rows].astype(F32) + self.inbox[rows].astype(F32)).astype(BF16)
            self.to_across(k).start()

    def finish(self, k):
        rows = self.rows(k)

        @pl.when(self.inner)
        def _():
            self.to_across(k).wait_recv()
            total = (self.mid[rows].astype(F32) + self.cross[rows].astype(F32)).astype(BF16)
            self.part[rows] = total
            self.to_pair(k).start()
            self.use(rows, total)

        @pl.when(self.outer)
        def _():
            self.to_pair(k).wait_recv()
            self.use(rows, self.inbox[rows])

    def drain(self):
        for k in range(CHUNKS):
            self.to_pair(k).wait_send()

        @pl.when(self.inner)
        def _():
            for k in range(CHUNKS):
                self.to_across(k).wait_send()


def _step_kernel(
    wq, wk, wv, wo, wd, wg, wu, bq, bk, bv, ga, gm, hid_hbm, lens_hbm, kc_hbm, vc_hbm,
    oq, ok, ov, oo, od, og, ou, obq, obk, obv, oga, ogm, kc, vc, out,
    sq, sk, sv, so, sd, sg, su, tq, tk, tv, tg, tu, dcut, vecs, hid, lens, kt, vt, aux, board, act, qt,
    score, total, down, part, inbox, mid, cross, part2, inbox2, mid2, cross2, x1,
    load_sem, vec_sem, own_sem, s0_send, s0_recv, s1_send, s1_recv, sp_send, sp_recv, aux_send, aux_recv,
    send1, recv1, send2, recv2,
):
    z, dp, core, col, cols, peers = _place()
    device = dp * TP + z
    own_here = z == col
    away = jnp.logical_not(own_here)
    at_peer = (dp, peers["x"], peers["y"], 2 * cols[3] + core)
    hbm = (wq, wk, wv, wo, wd, wg, wu)
    source = (sq, sk, sv, so, sd, sg, su)
    share = (oq, ok, ov, oo, down, og, ou)
    staged = {Q: tq, K: tk, V: tv, GATE: tg, UP: tu}

    loads = [pltpu.make_async_copy(src, dst, load_sem.at[i]) for i, (src, dst) in enumerate(
        zip(hbm + (hid_hbm, lens_hbm, kc_hbm, vc_hbm), source + (hid, lens, kc, vc)))]
    small = [pltpu.make_async_copy(src, vecs.at[i], vec_sem.at[i]) for i, src in enumerate((bq, bk, bv, ga, gm))]
    for copy in loads[:UP + 1] + small + loads[UP + 1:]:
        copy.start()

    barrier = pltpu.get_barrier_semaphore()
    for peer in (peers["x"], peers["y"], peers["d"], at_peer[3]):
        _signal(barrier, z, peer)
    for m in (1, 2, 3):
        _signal(barrier, (z + m) % TP, dp)

    for w in (Q, K, V):
        loads[w].wait()
    pl.semaphore_wait(barrier, 7)

    sent = []
    guarded = []

    def lanes_of(column):
        return _lanes(column * QUARTER, QUARTER)

    def root(w, plane_row):
        rows = source[w].shape[0]
        return lambda column: share[w].at[_rows((core * TP + plane_row) * rows, rows), lanes_of(column)]

    def own_piece(w):
        return pltpu.make_async_copy(hbm[w].at[:, lanes_of(col)], root(w, z)(col), own_sem.at[w])

    def scatter(w):
        for m in (1, 2, 3):
            src = source[w].at[:, lanes_of(cols[m])]
            sems = s0_send.at[w, m], s0_recv.at[w, m], z, at_peer[m]
            landing = _remote(src, root(w, z)(cols[m]), *sems)
            passing = _remote(src, staged[w].at[m], *sems)

            @pl.when(own_here)
            def _():
                landing.start()

            @pl.when(away)
            def _():
                passing.start()
            sent.append(passing)

        @pl.when(own_here)
        def _():
            own_piece(w).start()

    def forward(w):
        for m in range(4):
            piece = source[w].at[:, lanes_of(col)] if m == 0 else staged[w].at[m]
            copy = _remote(piece, root(w, z)(col), s1_send.at[w, m], s1_recv.at[w], cols[m], dp)
            if m:
                _remote(staged[w].at[m], staged[w].at[m], s0_send.at[w, m], s0_recv.at[w, m], z, dp).wait_recv()
            elsewhere = cols[m] != z

            @pl.when(elsewhere)
            def _():
                copy.start()
            guarded.append((elsewhere, copy))

    def columns(w, piece, dst):
        for m in (1, 2, 3):
            plane = (z + m) % TP
            copy = _remote(piece(plane), dst, s1_send.at[w, m], s1_recv.at[w], plane, dp)
            copy.start()
            sent.append(copy)

    def got_root(w):
        rows = source[w].shape[0]
        width = QUARTER if w in ROW_SHARED else share[w].shape[1]
        three = share[w].at[pl.ds(0, 3 * rows), pl.ds(0, width)]
        _remote(three, three, s1_send.at[w, 1], s1_recv.at[w], z, peers["x"]).wait_recv()
        if w in ROW_SHARED:
            @pl.when(own_here)
            def _():
                own_piece(w).wait()

    def rows_spread(w, index):
        ref, size = share[w], TP * source[w].shape[0]
        return _Spread(
            z, dp, cols, peers,
            ref.at[_rows(core * size, size), lanes_of(col)],
            lambda column: ref.at[_rows(core * size, size), lanes_of(column)],
            lambda column, half: ref.at[_rows(core * size + size // 2 * half, size // 2), lanes_of(column)],
            ref.at[_rows((1 - core) * size, size), :],
            sp_send.at[index], sp_recv.at[index])

    def columns_spread(w, index):
        ref = share[w]
        return _Spread(
            z, dp, cols, peers,
            ref.at[_rows(dp * LANES, LANES), :],
            lambda column: ref.at[_rows((2 * column + core) * LANES, LANES), :],
            lambda column, half: ref.at[_rows((2 * column + core) * LANES + HEAD * half, HEAD), :],
            ref.at[pl.ds(0, WIDTH // 2), :],
            sp_send.at[index], sp_recv.at[index])

    spreads = [(rows_spread if w in ROW_SHARED else columns_spread)(w, w) for w in range(7)]

    for w in (Q, K, V):
        scatter(w)
    out_rows = oo.at[_rows(dp * LANES + z * BLOCK, BLOCK), :]
    out_own = pltpu.make_async_copy(wo.at[:, lanes_of(z)], out_rows, own_sem.at[OUT])
    out_own.start()
    loads[OUT].wait()
    columns(OUT, lambda plane: so.at[:, lanes_of(plane)], out_rows)
    for w in (GATE, UP):
        loads[w].wait()
        scatter(w)

    for copy in small:
        copy.wait()
    spots = [(_lane((BLOCK, LANES)) == _sublane((BLOCK, LANES)) + BLOCK * r).astype(BF16) for r in range(TP)]
    aux[0] = sum(_dot(vecs[r], spot, 1, 0) for r, spot in enumerate(spots))
    aux[1] = _dot(vecs[TP], spots[0], 1, 0)
    board[pl.ds(device, 1)] = aux[...].reshape(1, 2, 1, LANES)
    for m in (1, 2, 3):
        _remote(aux, board.at[device], aux_send.at[0], aux_recv.at[0], (z + m) % TP, dp).start()
    y = col // 2
    steps = ((TP * dp, TP, "d"), (2 * TP * col, 2 * TP, "x"), (4 * TP * y, 4 * TP, "y"))

    def board_got(index, size, sending):
        part = board.at[pl.ds(0, size)]
        copy = _remote(part, part, aux_send.at[index], aux_recv.at[index], z, peers["x"])
        copy.wait_send() if sending else copy.wait_recv()

    def board_step(index):
        start, size, peer = steps[index]
        board_got(index, size // 2 if index else 3, False)
        part = board.at[pl.ds(start, size)]
        _remote(part, part, aux_send.at[index + 1], aux_recv.at[index + 1], z, peers[peer]).start()

    loads[DOWN].wait()
    for t in range(TP):
        dcut[t, :, :FF] = sd[:, FF * t:FF * (t + 1)]
        dcut[t, :, FF:] = jnp.zeros((BLOCK, FF_PAD - FF), BF16)
    down_rows = down.at[_rows(dp * LANES + z * BLOCK, BLOCK), :]
    down_rows[...] = dcut[z]

    for w in (Q, K, V):
        forward(w)
    board_step(0)
    columns(DOWN, lambda plane: dcut.at[plane], down_rows)
    out_own.wait()
    got_root(OUT)
    spreads[OUT].first()
    forward(GATE)
    board_step(1)
    got_root(Q)
    spreads[Q].first()
    forward(UP)
    for w in (K, V):
        got_root(w)
        spreads[w].first()
    board_step(2)
    spreads[Q].second()
    spreads[OUT].second()
    spreads[K].second()
    spreads[V].second()
    board_got(3, 4 * TP, False)

    sub = _sublane((BLOCK, LANES))
    first, second = jnp.zeros((BLOCK, LANES), F32), jnp.zeros((BLOCK, LANES), F32)
    for i in range(TP * DP):
        first = jnp.where(sub == i, board[i, 0], first)
        second = jnp.where(sub == i, board[i, 1], second)
    first, second = first.astype(BF16), second.astype(BF16)

    def spread_row(table, offset, count, keep):
        width = count * BLOCK
        spot = (_sublane((LANES, width)) == _lane((LANES, width)) % BLOCK + offset).astype(BF16)
        wide = _dot(table, spot, 1, 0)
        mine = _sublane((BLOCK, width)) == keep + _lane((BLOCK, width)) // BLOCK
        return jnp.sum(jnp.where(mine, wide, 0.0), axis=0, keepdims=True)

    gain_row = spread_row(first, 3 * BLOCK, TP * DP, 0)
    gain_mlp = spread_row(second, 0, TP * DP, 0)
    oga[...] = gain_row.astype(BF16).reshape(oga.shape)
    ogm[...] = gain_mlp.astype(BF16).reshape(ogm.shape)
    for r, ref in enumerate((obq, obk, obv)):
        ref[...] = spread_row(first, BLOCK * r, DP, DP * z).astype(BF16).reshape(ref.shape)

    def bias_column(r):
        tall_shape = (QUARTER, BLOCK)
        pick = (_lane(tall_shape) == DP * z + _sublane(tall_shape) // BLOCK).astype(BF16)
        tall = _dot(pick, first, 1, 0)
        mine = _lane(tall.shape) == BLOCK * r + _sublane(tall.shape) % BLOCK
        return jnp.sum(jnp.where(mine, tall, 0.0), axis=1, keepdims=True)

    for copy in loads[UP + 1:UP + 3]:
        copy.wait()
    act[...] = _rms(hid[...], gain_row)

    lens_row = lens[...]
    inv_freq = jnp.exp(_sublane((HALF, QUARTER)).astype(F32) * (-math.log(THETA) / HALF))
    angle = lens_row.astype(F32) * inv_freq
    cosine, sine = jnp.cos(angle), jnp.sin(angle)

    spreads[Q].third()
    got_root(DOWN)
    spreads[DOWN].first()
    spreads[K].third()

    def project(weight, r):
        return (_dot(weight[...], act[...], 1, 1) + bias_column(r)).astype(BF16)

    def rotate(vec, out):
        vec = vec.astype(F32)
        for h in range(TP):
            base = HEAD * h
            lo, hi = vec[base:base + HALF], vec[base + HALF:base + HEAD]
            out[base:base + HALF] = (lo * cosine - hi * sine).astype(BF16).astype(out.dtype)
            out[base + HALF:base + HEAD] = (hi * cosine + lo * sine).astype(BF16).astype(out.dtype)

    spreads[Q].last()
    rotate(project(oq, Q), qt)
    spreads[V].third()
    spreads[K].last()
    rotate(project(ok, K), kt)
    got_root(GATE)
    spreads[GATE].first()
    for copy in loads[UP + 3:]:
        copy.wait()

    def heads(h):
        return slice(HEAD * h, HEAD * (h + 1))

    def chunk_rows(chunk):
        return pl.ds(pl.multiple_of(chunk * SLOTS, SLOTS), SLOTS)

    def scores(start, stop):
        @pl.loop(start, stop)
        def _(chunk):
            for h in range(TP):
                query = qt[heads(h)]
                score[h, chunk_rows(chunk)] = jnp.concatenate([
                    jnp.sum(kc[chunk * SLOTS + i, h].astype(F32) * query, axis=0, keepdims=True)
                    for i in range(SLOTS)], axis=0)

    def values(half):
        @pl.loop(0, count)
        def _(chunk):
            for h in range(TP):
                weights = score[h, chunk_rows(chunk), half]
                acc = total[heads(h), half]
                for i in range(SLOTS):
                    acc = acc + vc[chunk * SLOTS + i, h, :, half].astype(F32) * weights[i:i + 1]
                total[heads(h), half] = acc

    def after_first(rows, total_rows):
        x1[rows] = (hid[rows].astype(F32) + total_rows.astype(F32)).astype(BF16)

    def after_second(rows, total_rows):
        out[rows] = (x1[rows].astype(F32) + total_rows.astype(F32)).astype(BF16)

    line1 = _LineSum(part, inbox, mid, cross, send1, recv1, after_first)
    line2 = _LineSum(part2, inbox2, mid2, cross2, send2, recv2, after_second)

    def attend(index):
        half = slice(LANES * index, LANES * (index + 1))
        slot = _sublane((kc.shape[0], LANES))
        lens_half = lens_row[:, half]
        for h in range(TP):
            fresh = jnp.sum(kt[heads(h), half].astype(F32) * qt[heads(h), half], axis=0, keepdims=True)
            raw = jnp.where(slot == lens_half, fresh, score[h, :, half]) * (HEAD ** -0.5)
            raw = jnp.where(slot <= lens_half, raw, -1e30)
            weight = jnp.exp(raw - jnp.max(raw, axis=0, keepdims=True))
            weight = (weight / jnp.sum(weight, axis=0, keepdims=True)).astype(BF16).astype(F32)
            newest = jnp.sum(jnp.where(slot == lens_half, weight, 0.0), axis=0, keepdims=True)
            score[h, :, half] = jnp.where(slot == lens_half, 0.0, weight)
            total[heads(h), half] = vt[heads(h), half].astype(F32) * newest
        values(half)
        part[half] = _dot(total[:, half].T.astype(BF16), oo[...], 1, 1).astype(BF16)
        for k in range(CHUNKS // 2 * index, CHUNKS // 2 * (index + 1)):
            line1.push(k)

    count = kc.shape[0] // SLOTS
    scores(0, count // 2)
    spreads[OUT].third()
    spreads[DOWN].second()
    scores(count // 2, count)
    spreads[V].last()
    vt[...] = project(ov, V)
    got_root(UP)
    spreads[UP].first()
    spreads[OUT].last()
    attend(0)
    attend(1)
    spreads[GATE].second()

    lens_b = lens_row.astype(F32).astype(BF16)

    def update(cache, new):
        @pl.loop(0, kc.shape[0])
        def _(slot):
            here = lens_b == slot.astype(F32).astype(BF16)
            for h in range(TP):
                cache[slot, h] = jnp.where(here, new[heads(h)], cache[slot, h])

    update(kc, kt)
    spreads[DOWN].third()

    def mlp(block):
        size = BLOCK_CHUNKS * CHUNK
        rows = pl.ds(block * size, size)
        norm = _rms(x1[rows], gain_mlp)
        gate = _dot(norm, og[...], 1, 1).astype(BF16).astype(F32)
        up = _dot(norm, ou[...], 1, 1).astype(BF16).astype(F32)
        gated = (jax.nn.silu(gate) * up).astype(BF16)
        part2[rows] = _dot(gated, down[:, :FF], 1, 1).astype(BF16)
        for k in range(block * BLOCK_CHUNKS, (block + 1) * BLOCK_CHUNKS):
            line2.push(k)

    def finish_first(k):
        line1.finish(k)
        if k == 1:
            for w in (GATE, UP, DOWN):
                spreads[w].last()
        if (k + 1) % BLOCK_CHUNKS == 0:
            mlp(k // BLOCK_CHUNKS)
        if k == CHUNKS - 1 - BLOCK_CHUNKS:
            for early in range(BLOCK_CHUNKS):
                line2.join(early)

    for k in range(CHUNKS):
        line1.join(k)
        if k == 0:
            spreads[UP].second()
        if k == 1:
            update(vc, vt)
            spreads[GATE].third()
        if k == LAG:
            spreads[UP].third()
        if k >= LAG:
            finish_first(k - LAG)
    for k in range(CHUNKS - LAG, CHUNKS):
        finish_first(k)
    for k in range(BLOCK_CHUNKS, CHUNKS):
        line2.join(k)
        if k == CHUNKS - 1:
            od[...] = down[...].T[:FF]
        if k >= LAG:
            line2.finish(k - LAG)
    for k in range(CHUNKS - LAG, CHUNKS):
        line2.finish(k)

    line1.drain()
    line2.drain()
    for copy in sent:
        copy.wait_send()
    for elsewhere, copy in guarded:
        @pl.when(elsewhere)
        def _():
            copy.wait_send()
    for spread in spreads:
        spread.drain()
    for index, size in enumerate((3, TP, 2 * TP, 4 * TP)):
        board_got(index, size, True)


def _step(weights, vectors, hid, lens, kc, vc):
    vmem = pl.BlockSpec(memory_space=pltpu.VMEM)
    anywhere = pl.BlockSpec(memory_space=pltpu.HBM)
    square = (QUARTER, QUARTER)
    sizes = [(QUARTER, WIDTH)] * 3 + [(WIDTH, QUARTER)] + [(FF, WIDTH)] * 3
    sizes += [(QUARTER,)] * 3 + [(WIDTH,)] * 2 + [kc.shape, vc.shape, hid.shape]
    outs = [pltpu.VMEM(size, BF16) for size in sizes]
    dma = pltpu.SemaphoreType.DMA
    inputs = [_in_hbm(a) for a in (*weights, *vectors, hid, lens, kc, vc)]
    rows = pltpu.VMEM(hid.shape, BF16)
    return pl.pallas_call(
        _step_kernel,
        out_shape=outs,
        in_specs=[anywhere] * len(inputs),
        out_specs=[vmem] * len(outs),
        scratch_shapes=[pltpu.VMEM(w.shape, BF16) for w in weights]
        + [pltpu.VMEM((4, weights[w].shape[0], QUARTER), BF16) for w in ROW_SHARED] + [
            pltpu.VMEM((TP, BLOCK, FF_PAD), BF16), pltpu.VMEM((5, 1, BLOCK), BF16), rows,
            pltpu.VMEM(lens.shape, lens.dtype), pltpu.VMEM(square, BF16), pltpu.VMEM(square, BF16),
            pltpu.VMEM((2, 1, LANES), F32), pltpu.VMEM((TP * DP, 2, 1, LANES), F32), rows, pltpu.VMEM(square, F32),
            pltpu.VMEM((TP, kc.shape[0], QUARTER), F32), pltpu.VMEM(square, F32),
            pltpu.VMEM((WIDTH, FF_PAD), BF16)]
        + [rows] * 9 + [
            dma((11,)), dma((5,)), dma((7,)), dma((7, 4)), dma((7, 4)), dma((7, 4)), dma((7,)),
            dma((7, SPREAD_SENDS)), dma((7, SPREAD_RECVS)), dma((4,)), dma((4,))] + [dma((2, CHUNKS))] * 4,
        compiler_params=pltpu.CompilerParams(collective_id=0, has_side_effects=True, vmem_limit_bytes=24 * MIB),
        cost_estimate=pl.CostEstimate(flops=2 * 10**10, bytes_accessed=MIB, transcendentals=0),
        name="step",
    )(*inputs)


def _emit_kernel(*refs):
    count = len(refs) // 2
    copies = [pltpu.make_async_copy(refs[i], refs[count + i], refs[-1].at[i]) for i in range(count)]
    for copy in copies:
        copy.start()
    for copy in copies:
        copy.wait()


def _emit(arrays):
    vmem, hbm = pl.BlockSpec(memory_space=pltpu.VMEM), pl.BlockSpec(memory_space=pltpu.HBM)
    return pl.pallas_call(
        _emit_kernel,
        out_shape=[jax.ShapeDtypeStruct(a.shape, BF16) for a in arrays],
        in_specs=[vmem] * len(arrays),
        out_specs=[hbm] * len(arrays),
        scratch_shapes=[pltpu.SemaphoreType.DMA((len(arrays),))],
        compiler_params=pltpu.CompilerParams(vmem_limit_bytes=4 * MIB),
        cost_estimate=pl.CostEstimate(flops=10**9, bytes_accessed=24 * MIB, transcendentals=0),
        name="emit",
    )(*arrays)


def solution(mesh):
    def local_step(wq, bq, wk, bk, wv, bv, wo, wg, wu, wd, ga, gm, hid, k_cache, v_cache, lengths):
        vectors = [v.reshape(1, -1) for v in (bq, bk, bv, ga, gm)]
        kc, vc = jnp.transpose(k_cache, (1, 2, 3, 0)), jnp.transpose(v_cache, (1, 2, 3, 0))
        (gq, gk, gv, go, gd, gg, gu, gbq, gbk, gbv, gga, ggm, kc_v, vc_v, out_v) = _step(
            (wq, wk, wv, wo, wd, wg, wu), vectors, hid, lengths.reshape(1, -1), kc, vc)
        ko, vo, og, ou, od, oq, ok, ov, oo, out, obq, obk, obv, oga, ogm = _emit(
            (kc_v, vc_v, gg, gu, gd, gq, gk, gv, go, out_v, gbq, gbk, gbv, gga, ggm))
        return (oq, obq, ok, obk, ov, obv, oo, og, ou, od.T, oga, ogm, out,
                jnp.transpose(ko, (3, 0, 1, 2)), jnp.transpose(vo, (3, 0, 1, 2)))

    row_spec = P(("dp", "tp"), None)
    flat_spec = P(("dp", "tp"))
    cache_spec = P("dp", None, "tp", None)
    in_specs = (row_spec, flat_spec, row_spec, flat_spec, row_spec, flat_spec, row_spec, row_spec, row_spec, row_spec,
                flat_spec, flat_spec, P("dp", None), cache_spec, cache_spec, P("dp"))
    out_specs = (P("tp", None), P("tp"), P("tp", None), P("tp"), P("tp", None), P("tp"), P(None, "tp"), P("tp", None),
                 P("tp", None), P(None, "tp"), P(None), P(None), P("dp", None), cache_spec, cache_spec)
    return jax.shard_map(local_step, mesh=mesh, in_specs=in_specs, out_specs=out_specs, check_vma=False)
```

```python
import math

import jax
import jax.numpy as jnp
from jax import lax
from jax.experimental import pallas as pl
from jax.experimental.pallas import tpu as pltpu
from jax.sharding import PartitionSpec as P

EPS = 1e-6
THETA = 1000000.0
MESH = pl.DeviceIdType.MESH
BF16, F32 = jnp.bfloat16, jnp.float32
TP, DP = 4, 8
HEAD, HALF = 64, 32
WIDTH, QUARTER, LANES = 1024, 256, 128
BLOCK, WIDE_BLOCK = 32, 88
FF, FF_PAD = 704, 768
MIB = 2**20


def _place():
    z, dp = lax.axis_index("tp"), lax.axis_index("dp")
    core, col = dp % 2, dp // 2
    x, y = col % 2, col // 2
    cols = (col, col + 1 - 2 * x, col + 2 - 4 * y, 3 - col)
    peers = {"x": dp + 2 - 4 * x, "y": dp + 4 - 8 * y, "d": dp + 1 - 2 * core}
    return z, dp, core, col, cols, peers


def _remote(src, dst, send, recv, tp, dp):
    return pltpu.make_async_remote_copy(
        src_ref=src, dst_ref=dst, send_sem=send, recv_sem=recv, device_id={"tp": tp, "dp": dp}, device_id_type=MESH
    )


def _rows(start, size):
    return pl.ds(pl.multiple_of(start, 8), size)


def _lanes(start, size):
    return pl.ds(pl.multiple_of(start, 128), size)


def _signal(sem, tp, dp):
    pl.semaphore_signal(sem, inc=1, device_id={"tp": tp, "dp": dp}, device_id_type=MESH)


def _dot(a, b, ca, cb):
    return lax.dot_general(a, b, (((ca,), (cb,)), ((), ())), preferred_element_type=F32)


def _iota(shape, axis):
    return lax.broadcasted_iota(jnp.int32, shape, axis)


def _sublane(shape):
    return _iota(shape, 0)


def _lane(shape):
    return _iota(shape, 1)


def _in_hbm(array):
    return pltpu.with_memory_space_constraint(array, pltpu.HBM)


def _rms(act, gain_row):
    act = act.astype(F32)
    inv = lax.rsqrt(jnp.mean(act * act, axis=-1, keepdims=True) + EPS)
    return (act * inv * gain_row).astype(BF16)


class _Spread:
    def __init__(self, tp, dp, cols, peers, src_own, region, halves, total, send, recv):
        self.tp, self.cols, self.peers = tp, cols, peers
        self.src_own, self.region, self.halves, self.total = src_own, region, halves, total
        self.send, self.recv = send, recv
        self.sent = []

    def _go(self, src, dst, peer, recv_index):
        copy = _remote(src, dst, self.send.at[len(self.sent)], self.recv.at[recv_index], self.tp, self.peers[peer])
        copy.start()
        self.sent.append(copy)

    def _got(self, ref, recv_index):
        _remote(ref, ref, self.send.at[0], self.recv.at[recv_index], self.tp, self.peers["x"]).wait_recv()

    def first(self):
        own = self.region(self.cols[0])
        self._go(self.src_own, own, "x", 0)
        self._go(self.src_own, own, "y", 1)
        self._go(self.src_own, own, "d", 4)

    def second(self):
        at_x, at_y = self.region(self.cols[1]), self.region(self.cols[2])
        self._got(at_x, 0)
        upper = self.halves(self.cols[1], 0)
        self._go(upper, upper, "y", 2)
        self._go(at_x, at_x, "d", 4)
        self._got(at_y, 1)
        lower = self.halves(self.cols[2], 1)
        self._go(lower, lower, "x", 3)
        self._go(at_y, at_y, "d", 4)

    def third(self):
        upper, lower = self.halves(self.cols[3], 0), self.halves(self.cols[3], 1)
        self._got(upper, 2)
        self._go(upper, upper, "d", 4)
        self._got(lower, 3)
        self._go(lower, lower, "d", 4)

    def last(self):
        self._got(self.total, 4)

    def drain(self):
        for copy in self.sent:
            copy.wait_send()


SPREAD_SENDS, SPREAD_RECVS = 9, 5
Q, K, V, OUT, DOWN, GATE, UP = range(7)
ROW_SHARED = (Q, K, V, GATE, UP)
SLOTS = 8
CHUNK = 32
CHUNKS = QUARTER // CHUNK
BLOCK_CHUNKS = 2
LAG = 2


class _LineSum:
    def __init__(self, part, inbox, mid, cross, send, recv, use):
        self.part, self.inbox, self.mid, self.cross, self.send, self.recv = part, inbox, mid, cross, send, recv
        z, dp = lax.axis_index("tp"), lax.axis_index("dp")
        self.pair, self.across, self.dp = z + 1 - 2 * (z % 2), TP - 1 - z, dp
        self.inner = jnp.logical_and(z >= 1, z <= 2)
        self.outer = jnp.logical_not(self.inner)
        self.use = use

    def rows(self, k):
        return pl.ds(k * CHUNK, CHUNK)

    def to_pair(self, k):
        return _remote(self.part.at[self.rows(k)], self.inbox.at[self.rows(k)], self.send.at[0, k],
                       self.recv.at[0, k], self.pair, self.dp)

    def to_across(self, k):
        return _remote(self.mid.at[self.rows(k)], self.cross.at[self.rows(k)], self.send.at[1, k], self.recv.at[1, k],
                       self.across, self.dp)

    def push(self, k):
        @pl.when(self.outer)
        def _():
            self.to_pair(k).start()

    def join(self, k):
        @pl.when(self.inner)
        def _():
            rows = self.rows(k)
            self.to_pair(k).wait_recv()
            self.mid[rows] = (self.part[rows].astype(F32) + self.inbox[rows].astype(F32)).astype(BF16)
            self.to_across(k).start()

    def finish(self, k):
        rows = self.rows(k)

        @pl.when(self.inner)
        def _():
            self.to_across(k).wait_recv()
            total = (self.mid[rows].astype(F32) + self.cross[rows].astype(F32)).astype(BF16)
            self.part[rows] = total
            self.to_pair(k).start()
            self.use(rows, total)

        @pl.when(self.outer)
        def _():
            self.to_pair(k).wait_recv()
            self.use(rows, self.inbox[rows])

    def drain(self):
        for k in range(CHUNKS):
            self.to_pair(k).wait_send()

        @pl.when(self.inner)
        def _():
            for k in range(CHUNKS):
                self.to_across(k).wait_send()


def _step_kernel(
    wq, wk, wv, wo, wd, wg, wu, bq, bk, bv, ga, gm, hid_hbm, lens_hbm, kc_hbm, vc_hbm,
    oq, ok, ov, oo, od, og, ou, obq, obk, obv, oga, ogm, kc, vc, out,
    sq, sk, sv, so, sd, sg, su, tq, tk, tv, tg, tu, dcut, vecs, hid, lens, kt, vt, aux, board, act, qt,
    score, total, down, part, inbox, mid, cross, part2, inbox2, mid2, cross2, x1,
    load_sem, vec_sem, own_sem, s0_send, s0_recv, s1_send, s1_recv, sp_send, sp_recv, aux_send, aux_recv,
    send1, recv1, send2, recv2,
):
    z, dp, core, col, cols, peers = _place()
    device = dp * TP + z
    own_here = z == col
    away = jnp.logical_not(own_here)
    at_peer = (dp, peers["x"], peers["y"], 2 * cols[3] + core)
    hbm = (wq, wk, wv, wo, wd, wg, wu)
    source = (sq, sk, sv, so, sd, sg, su)
    share = (oq, ok, ov, oo, down, og, ou)
    staged = {Q: tq, K: tk, V: tv, GATE: tg, UP: tu}

    loads = [pltpu.make_async_copy(src, dst, load_sem.at[i]) for i, (src, dst) in enumerate(
        zip(hbm + (hid_hbm, lens_hbm, kc_hbm, vc_hbm), source + (hid, lens, kc, vc)))]
    small = [pltpu.make_async_copy(src, vecs.at[i], vec_sem.at[i]) for i, src in enumerate((bq, bk, bv, ga, gm))]
    for copy in loads[:UP + 1] + small + loads[UP + 1:]:
        copy.start()

    barrier = pltpu.get_barrier_semaphore()
    for peer in (peers["x"], peers["y"], peers["d"], at_peer[3]):
        _signal(barrier, z, peer)
    for m in (1, 2, 3):
        _signal(barrier, (z + m) % TP, dp)

    for w in (Q, K, V):
        loads[w].wait()
    pl.semaphore_wait(barrier, 7)

    sent = []
    guarded = []

    def lanes_of(column):
        return _lanes(column * QUARTER, QUARTER)

    def root(w, plane_row):
        rows = source[w].shape[0]
        return lambda column: share[w].at[_rows((core * TP + plane_row) * rows, rows), lanes_of(column)]

    def own_piece(w):
        return pltpu.make_async_copy(hbm[w].at[:, lanes_of(col)], root(w, z)(col), own_sem.at[w])

    def scatter(w):
        for m in (1, 2, 3):
            src = source[w].at[:, lanes_of(cols[m])]
            sems = s0_send.at[w, m], s0_recv.at[w, m], z, at_peer[m]
            landing = _remote(src, root(w, z)(cols[m]), *sems)
            passing = _remote(src, staged[w].at[m], *sems)

            @pl.when(own_here)
            def _():
                landing.start()

            @pl.when(away)
            def _():
                passing.start()
            sent.append(passing)

        @pl.when(own_here)
        def _():
            own_piece(w).start()

    def forward(w):
        for m in range(4):
            piece = source[w].at[:, lanes_of(col)] if m == 0 else staged[w].at[m]
            copy = _remote(piece, root(w, z)(col), s1_send.at[w, m], s1_recv.at[w], cols[m], dp)
            if m:
                _remote(staged[w].at[m], staged[w].at[m], s0_send.at[w, m], s0_recv.at[w, m], z, dp).wait_recv()
            elsewhere = cols[m] != z

            @pl.when(elsewhere)
            def _():
                copy.start()
            guarded.append((elsewhere, copy))

    def columns(w, piece, dst):
        for m in (1, 2, 3):
            plane = (z + m) % TP
            copy = _remote(piece(plane), dst, s1_send.at[w, m], s1_recv.at[w], plane, dp)
            copy.start()
            sent.append(copy)

    def got_root(w):
        rows = source[w].shape[0]
        width = QUARTER if w in ROW_SHARED else share[w].shape[1]
        three = share[w].at[pl.ds(0, 3 * rows), pl.ds(0, width)]
        _remote(three, three, s1_send.at[w, 1], s1_recv.at[w], z, peers["x"]).wait_recv()
        if w in ROW_SHARED:
            @pl.when(own_here)
            def _():
                own_piece(w).wait()

    def rows_spread(w, index):
        ref, size = share[w], TP * source[w].shape[0]
        return _Spread(
            z, dp, cols, peers,
            ref.at[_rows(core * size, size), lanes_of(col)],
            lambda column: ref.at[_rows(core * size, size), lanes_of(column)],
            lambda column, half: ref.at[_rows(core * size + size // 2 * half, size // 2), lanes_of(column)],
            ref.at[_rows((1 - core) * size, size), :],
            sp_send.at[index], sp_recv.at[index])

    def columns_spread(w, index):
        ref = share[w]
        return _Spread(
            z, dp, cols, peers,
            ref.at[_rows(dp * LANES, LANES), :],
            lambda column: ref.at[_rows((2 * column + core) * LANES, LANES), :],
            lambda column, half: ref.at[_rows((2 * column + core) * LANES + HEAD * half, HEAD), :],
            ref.at[pl.ds(0, WIDTH // 2), :],
            sp_send.at[index], sp_recv.at[index])

    spreads = [(rows_spread if w in ROW_SHARED else columns_spread)(w, w) for w in range(7)]

    for w in (Q, K, V):
        scatter(w)
    out_rows = oo.at[_rows(dp * LANES + z * BLOCK, BLOCK), :]
    out_own = pltpu.make_async_copy(wo.at[:, lanes_of(z)], out_rows, own_sem.at[OUT])
    out_own.start()
    loads[OUT].wait()
    columns(OUT, lambda plane: so.at[:, lanes_of(plane)], out_rows)
    for w in (GATE, UP):
        loads[w].wait()
        scatter(w)

    for copy in small:
        copy.wait()
    spots = [(_lane((BLOCK, LANES)) == _sublane((BLOCK, LANES)) + BLOCK * r).astype(BF16) for r in range(TP)]
    aux[0] = sum(_dot(vecs[r], spot, 1, 0) for r, spot in enumerate(spots))
    aux[1] = _dot(vecs[TP], spots[0], 1, 0)
    board[pl.ds(device, 1)] = aux[...].reshape(1, 2, 1, LANES)
    for m in (1, 2, 3):
        _remote(aux, board.at[device], aux_send.at[0], aux_recv.at[0], (z + m) % TP, dp).start()
    y = col // 2
    steps = ((TP * dp, TP, "d"), (2 * TP * col, 2 * TP, "x"), (4 * TP * y, 4 * TP, "y"))

    def board_got(index, size, sending):
        part = board.at[pl.ds(0, size)]
        copy = _remote(part, part, aux_send.at[index], aux_recv.at[index], z, peers["x"])
        copy.wait_send() if sending else copy.wait_recv()

    def board_step(index):
        start, size, peer = steps[index]
        board_got(index, size // 2 if index else 3, False)
        part = board.at[pl.ds(start, size)]
        _remote(part, part, aux_send.at[index + 1], aux_recv.at[index + 1], z, peers[peer]).start()

    loads[DOWN].wait()
    for t in range(TP):
        dcut[t, :, :FF] = sd[:, FF * t:FF * (t + 1)]
        dcut[t, :, FF:] = jnp.zeros((BLOCK, FF_PAD - FF), BF16)
    down_rows = down.at[_rows(dp * LANES + z * BLOCK, BLOCK), :]
    down_rows[...] = dcut[z]

    for w in (Q, K, V):
        forward(w)
    board_step(0)
    columns(DOWN, lambda plane: dcut.at[plane], down_rows)
    out_own.wait()
    got_root(OUT)
    spreads[OUT].first()
    forward(GATE)
    board_step(1)
    got_root(Q)
    spreads[Q].first()
    forward(UP)
    for w in (K, V):
        got_root(w)
        spreads[w].first()
    board_step(2)
    spreads[Q].second()
    spreads[OUT].second()
    spreads[K].second()
    spreads[V].second()
    board_got(3, 4 * TP, False)

    sub = _sublane((BLOCK, LANES))
    first, second = jnp.zeros((BLOCK, LANES), F32), jnp.zeros((BLOCK, LANES), F32)
    for i in range(TP * DP):
        first = jnp.where(sub == i, board[i, 0], first)
        second = jnp.where(sub == i, board[i, 1], second)
    first, second = first.astype(BF16), second.astype(BF16)

    def spread_row(table, offset, count, keep):
        width = count * BLOCK
        spot = (_sublane((LANES, width)) == _lane((LANES, width)) % BLOCK + offset).astype(BF16)
        wide = _dot(table, spot, 1, 0)
        mine = _sublane((BLOCK, width)) == keep + _lane((BLOCK, width)) // BLOCK
        return jnp.sum(jnp.where(mine, wide, 0.0), axis=0, keepdims=True)

    gain_row = spread_row(first, 3 * BLOCK, TP * DP, 0)
    gain_mlp = spread_row(second, 0, TP * DP, 0)
    oga[...] = gain_row.astype(BF16).reshape(oga.shape)
    ogm[...] = gain_mlp.astype(BF16).reshape(ogm.shape)
    for r, ref in enumerate((obq, obk, obv)):
        ref[...] = spread_row(first, BLOCK * r, DP, DP * z).astype(BF16).reshape(ref.shape)

    def bias_column(r):
        tall_shape = (QUARTER, BLOCK)
        pick = (_lane(tall_shape) == DP * z + _sublane(tall_shape) // BLOCK).astype(BF16)
        tall = _dot(pick, first, 1, 0)
        mine = _lane(tall.shape) == BLOCK * r + _sublane(tall.shape) % BLOCK
        return jnp.sum(jnp.where(mine, tall, 0.0), axis=1, keepdims=True)

    for copy in loads[UP + 1:UP + 3]:
        copy.wait()
    act[...] = _rms(hid[...], gain_row)

    lens_row = lens[...]
    inv_freq = jnp.exp(_sublane((HALF, QUARTER)).astype(F32) * (-math.log(THETA) / HALF))
    angle = lens_row.astype(F32) * inv_freq
    cosine, sine = jnp.cos(angle), jnp.sin(angle)

    spreads[Q].third()
    got_root(DOWN)
    spreads[DOWN].first()
    spreads[K].third()
    spreads[V].third()

    def project(weight, r):
        return (_dot(weight[...], act[...], 1, 1) + bias_column(r)).astype(BF16)

    def rotate(vec, out):
        vec = vec.astype(F32)
        for h in range(TP):
            base = HEAD * h
            lo, hi = vec[base:base + HALF], vec[base + HALF:base + HEAD]
            out[base:base + HALF] = (lo * cosine - hi * sine).astype(BF16).astype(out.dtype)
            out[base + HALF:base + HEAD] = (hi * cosine + lo * sine).astype(BF16).astype(out.dtype)

    spreads[Q].last()
    rotate(project(oq, Q), qt)
    spreads[K].last()
    rotate(project(ok, K), kt)
    got_root(GATE)
    spreads[GATE].first()
    for copy in loads[UP + 3:]:
        copy.wait()

    def heads(h):
        return slice(HEAD * h, HEAD * (h + 1))

    def chunk_rows(chunk):
        return pl.ds(pl.multiple_of(chunk * SLOTS, SLOTS), SLOTS)

    def scores(start, stop):
        @pl.loop(start, stop)
        def _(chunk):
            for h in range(TP):
                query = qt[heads(h)]
                score[h, chunk_rows(chunk)] = jnp.concatenate([
                    jnp.sum(kc[chunk * SLOTS + i, h].astype(F32) * query, axis=0, keepdims=True)
                    for i in range(SLOTS)], axis=0)

    def values(half):
        @pl.loop(0, count)
        def _(chunk):
            for h in range(TP):
                weights = score[h, chunk_rows(chunk), half]
                acc = total[heads(h), half]
                for i in range(SLOTS):
                    acc = acc + vc[chunk * SLOTS + i, h, :, half].astype(F32) * weights[i:i + 1]
                total[heads(h), half] = acc

    def after_first(rows, total_rows):
        x1[rows] = (hid[rows].astype(F32) + total_rows.astype(F32)).astype(BF16)

    def after_second(rows, total_rows):
        out[rows] = (x1[rows].astype(F32) + total_rows.astype(F32)).astype(BF16)

    line1 = _LineSum(part, inbox, mid, cross, send1, recv1, after_first)
    line2 = _LineSum(part2, inbox2, mid2, cross2, send2, recv2, after_second)

    def attend(index):
        half = slice(LANES * index, LANES * (index + 1))
        slot = _sublane((kc.shape[0], LANES))
        lens_half = lens_row[:, half]
        for h in range(TP):
            fresh = jnp.sum(kt[heads(h), half].astype(F32) * qt[heads(h), half], axis=0, keepdims=True)
            raw = jnp.where(slot == lens_half, fresh, score[h, :, half]) * (HEAD ** -0.5)
            raw = jnp.where(slot <= lens_half, raw, -1e30)
            weight = jnp.exp(raw - jnp.max(raw, axis=0, keepdims=True))
            weight = (weight / jnp.sum(weight, axis=0, keepdims=True)).astype(BF16).astype(F32)
            newest = jnp.sum(jnp.where(slot == lens_half, weight, 0.0), axis=0, keepdims=True)
            score[h, :, half] = jnp.where(slot == lens_half, 0.0, weight)
            total[heads(h), half] = vt[heads(h), half].astype(F32) * newest
        values(half)
        part[half] = _dot(total[:, half].T.astype(BF16), oo[...], 1, 1).astype(BF16)
        for k in range(CHUNKS // 2 * index, CHUNKS // 2 * (index + 1)):
            line1.push(k)

    count = kc.shape[0] // SLOTS
    scores(0, count // 2)
    spreads[OUT].third()
    spreads[DOWN].second()
    scores(count // 2, count)
    spreads[V].last()
    vt[...] = project(ov, V)
    got_root(UP)
    spreads[UP].first()
    spreads[OUT].last()
    attend(0)
    attend(1)
    spreads[GATE].second()

    lens_b = lens_row.astype(F32).astype(BF16)

    def update(cache, new):
        @pl.loop(0, kc.shape[0])
        def _(slot):
            here = lens_b == slot.astype(F32).astype(BF16)
            for h in range(TP):
                cache[slot, h] = jnp.where(here, new[heads(h)], cache[slot, h])

    update(kc, kt)
    spreads[DOWN].third()

    def mlp(block):
        size = BLOCK_CHUNKS * CHUNK
        rows = pl.ds(block * size, size)
        norm = _rms(x1[rows], gain_mlp)
        gate = _dot(norm, og[...], 1, 1).astype(BF16).astype(F32)
        up = _dot(norm, ou[...], 1, 1).astype(BF16).astype(F32)
        gated = (jax.nn.silu(gate) * up).astype(BF16)
        part2[rows] = _dot(gated, down[:, :FF], 1, 1).astype(BF16)
        for k in range(block * BLOCK_CHUNKS, (block + 1) * BLOCK_CHUNKS):
            line2.push(k)

    def finish_first(k):
        line1.finish(k)
        if k == 1:
            for w in (GATE, UP, DOWN):
                spreads[w].last()
        if (k + 1) % BLOCK_CHUNKS == 0:
            mlp(k // BLOCK_CHUNKS)
        if k == CHUNKS - 1 - BLOCK_CHUNKS:
            for early in range(BLOCK_CHUNKS):
                line2.join(early)

    for k in range(CHUNKS):
        line1.join(k)
        if k == 0:
            spreads[UP].second()
        if k == 1:
            update(vc, vt)
            spreads[GATE].third()
        if k == LAG:
            spreads[UP].third()
        if k >= LAG:
            finish_first(k - LAG)
    for k in range(CHUNKS - LAG, CHUNKS):
        finish_first(k)
    for k in range(BLOCK_CHUNKS, CHUNKS):
        line2.join(k)
        if k == CHUNKS - 1:
            od[...] = down[...].T[:FF]
        if k >= LAG:
            line2.finish(k - LAG)
    for k in range(CHUNKS - LAG, CHUNKS):
        line2.finish(k)

    line1.drain()
    line2.drain()
    for copy in sent:
        copy.wait_send()
    for elsewhere, copy in guarded:
        @pl.when(elsewhere)
        def _():
            copy.wait_send()
    for spread in spreads:
        spread.drain()
    for index, size in enumerate((3, TP, 2 * TP, 4 * TP)):
        board_got(index, size, True)


def _step(weights, vectors, hid, lens, kc, vc):
    vmem = pl.BlockSpec(memory_space=pltpu.VMEM)
    anywhere = pl.BlockSpec(memory_space=pltpu.HBM)
    square = (QUARTER, QUARTER)
    sizes = [(QUARTER, WIDTH)] * 3 + [(WIDTH, QUARTER)] + [(FF, WIDTH)] * 3
    sizes += [(QUARTER,)] * 3 + [(WIDTH,)] * 2 + [kc.shape, vc.shape, hid.shape]
    outs = [pltpu.VMEM(size, BF16) for size in sizes]
    dma = pltpu.SemaphoreType.DMA
    inputs = [_in_hbm(a) for a in (*weights, *vectors, hid, lens, kc, vc)]
    rows = pltpu.VMEM(hid.shape, BF16)
    return pl.pallas_call(
        _step_kernel,
        out_shape=outs,
        in_specs=[anywhere] * len(inputs),
        out_specs=[vmem] * len(outs),
        scratch_shapes=[pltpu.VMEM(w.shape, BF16) for w in weights]
        + [pltpu.VMEM((4, weights[w].shape[0], QUARTER), BF16) for w in ROW_SHARED] + [
            pltpu.VMEM((TP, BLOCK, FF_PAD), BF16), pltpu.VMEM((5, 1, BLOCK), BF16), rows,
            pltpu.VMEM(lens.shape, lens.dtype), pltpu.VMEM(square, BF16), pltpu.VMEM(square, BF16),
            pltpu.VMEM((2, 1, LANES), F32), pltpu.VMEM((TP * DP, 2, 1, LANES), F32), rows, pltpu.VMEM(square, F32),
            pltpu.VMEM((TP, kc.shape[0], QUARTER), F32), pltpu.VMEM(square, F32),
            pltpu.VMEM((WIDTH, FF_PAD), BF16)]
        + [rows] * 9 + [
            dma((11,)), dma((5,)), dma((7,)), dma((7, 4)), dma((7, 4)), dma((7, 4)), dma((7,)),
            dma((7, SPREAD_SENDS)), dma((7, SPREAD_RECVS)), dma((4,)), dma((4,))] + [dma((2, CHUNKS))] * 4,
        compiler_params=pltpu.CompilerParams(collective_id=0, has_side_effects=True, vmem_limit_bytes=24 * MIB),
        cost_estimate=pl.CostEstimate(flops=2 * 10**10, bytes_accessed=MIB, transcendentals=0),
        name="step",
    )(*inputs)


def _emit_kernel(*refs):
    count = len(refs) // 2
    copies = [pltpu.make_async_copy(refs[i], refs[count + i], refs[-1].at[i]) for i in range(count)]
    for copy in copies:
        copy.start()
    for copy in copies:
        copy.wait()


def _emit(arrays):
    vmem, hbm = pl.BlockSpec(memory_space=pltpu.VMEM), pl.BlockSpec(memory_space=pltpu.HBM)
    return pl.pallas_call(
        _emit_kernel,
        out_shape=[jax.ShapeDtypeStruct(a.shape, BF16) for a in arrays],
        in_specs=[vmem] * len(arrays),
        out_specs=[hbm] * len(arrays),
        scratch_shapes=[pltpu.SemaphoreType.DMA((len(arrays),))],
        compiler_params=pltpu.CompilerParams(vmem_limit_bytes=4 * MIB),
        cost_estimate=pl.CostEstimate(flops=10**9, bytes_accessed=24 * MIB, transcendentals=0),
        name="emit",
    )(*arrays)


def solution(mesh):
    def local_step(wq, bq, wk, bk, wv, bv, wo, wg, wu, wd, ga, gm, hid, k_cache, v_cache, lengths):
        vectors = [v.reshape(1, -1) for v in (bq, bk, bv, ga, gm)]
        kc, vc = jnp.transpose(k_cache, (1, 2, 3, 0)), jnp.transpose(v_cache, (1, 2, 3, 0))
        (gq, gk, gv, go, gd, gg, gu, gbq, gbk, gbv, gga, ggm, kc_v, vc_v, out_v) = _step(
            (wq, wk, wv, wo, wd, wg, wu), vectors, hid, lengths.reshape(1, -1), kc, vc)
        ko, vo, og, ou, od, oq, ok, ov, oo, out, obq, obk, obv, oga, ogm = _emit(
            (kc_v, vc_v, gg, gu, gd, gq, gk, gv, go, out_v, gbq, gbk, gbv, gga, ggm))
        return (oq, obq, ok, obk, ov, obv, oo, og, ou, od.T, oga, ogm, out,
                jnp.transpose(ko, (3, 0, 1, 2)), jnp.transpose(vo, (3, 0, 1, 2)))

    row_spec = P(("dp", "tp"), None)
    flat_spec = P(("dp", "tp"))
    cache_spec = P("dp", None, "tp", None)
    in_specs = (row_spec, flat_spec, row_spec, flat_spec, row_spec, flat_spec, row_spec, row_spec, row_spec, row_spec,
                flat_spec, flat_spec, P("dp", None), cache_spec, cache_spec, P("dp"))
    out_specs = (P("tp", None), P("tp"), P("tp", None), P("tp"), P("tp", None), P("tp"), P(None, "tp"), P("tp", None),
                 P("tp", None), P(None, "tp"), P(None), P(None), P("dp", None), cache_spec, cache_spec)
    return jax.shard_map(local_step, mesh=mesh, in_specs=in_specs, out_specs=out_specs, check_vma=False)
```
